32 devices in a mesh: dp: 8 (over z, y), mp: 4 (over x, core).
Axes of the slice: x: 2, y: 2, z: 4, core: 2. Of those that a mesh axis runs over, the one named last changes fastest.
Arguments:
- queries: bfloat16 [64, 64, 128], P('dp', 'mp'), may hold values from -140 to 140
- resident_cache: bfloat16 [64, 256, 8, 128], P('dp', None, 'mp'), may hold values from -6 to 6
- overflow_cache: bfloat16 [8, 8, 8, 128, 8, 128], P('dp', None, None, None, 'mp'), may hold values from -6 to 6
- key_up_weight: bfloat16 [8, 64, 128], P('mp'), may hold values from -0.75 to 0.75
- value_up_weight: bfloat16 [8, 64, 128], P('mp'), may hold values from -0.75 to 0.75
- lengths: int32 [64], replicated, may hold values from 257 to 1024
- routes: int32 [64, 6, 1], replicated, may hold values from 0 to 7; in each aligned block of 48 rows (0 to 47, 48 to 95, ..., all dimensions but the last counted through in order) at most 8 rows name the same one
- out_weight: bfloat16 [8192, 8192], P('mp', 'dp'), may hold values from -0.0625 to 0.0625
Outputs:
- mixed_out: bfloat16 [64, 8192], P('mp', 'dp')
The draws below stay inside these ranges and needn't reach their ends.
Inputs may be any that keep to these rules, and one draw needn't show every extreme that they name: Among the 48 entries of one sequence group (sequences s with the same s // 8) no group is named more than 8 times; the page named by routes[s, j, 0] lies in the slots of that holding group kept for the group s // 8, at the slot given by ranking. Slots that no entry names hold data that no output reads.
All inputs are finite; a program needn't handle non-finite values.
Results may differ from the reference program's by a relative error of at most 0.0049.
Values may be sent and summed in bfloat16 or wider, within the bound.
No kernel may reach another device: no remote copies, remote signals or barrier semaphores. Data moves between devices by JAX's collectives and lax.ppermute only.
A program may use at most 64 MiB of HBM per device.

```python
import math
import jax
import jax.numpy as jnp
import numpy as np
from jax import lax

D = 8192
QUERY_HEADS = 64
KEY_VALUE_HEADS = 8
HEAD_DIMENSION = 128
KEY_LATENT_RANK = 64
VALUE_LATENT_RANK = 64
PAGE_TOKENS = 128
RESIDENT_PAGES = 2
REMOTE_PAGES = 6
SEQ_DEV = 8
SEQUENCE_TOTAL = 64
SPILL_CAPACITY = 8
N_DP = 8


def draw_queries(key, part):
    shape = (SEQUENCE_TOTAL, QUERY_HEADS, HEAD_DIMENSION)
    first_key = jax.random.fold_in(key, 0)
    values = jnp.clip(jax.random.normal(first_key, shape, jnp.float32), -4.0, 4.0)
    return values.astype(jnp.bfloat16)


def with_ends(entries, stream_key, smallest, largest):
    place = [jax.random.randint(jax.random.fold_in(stream_key, axis), (), 0, length) for axis, length in enumerate(entries.shape)]
    main_axis = entries.shape.index(max(entries.shape))
    beside = place[:main_axis] + [(place[main_axis] + 1) % entries.shape[main_axis]] + place[main_axis + 1:]
    return entries.at[tuple(place)].set(smallest).at[tuple(beside)].set(largest)


def block_scale(stream_key, dims, cuts, low, top_value):
    loudness = 1.0
    for dim, shards_of in cuts:
        steps = jax.random.uniform(jax.random.fold_in(jax.random.fold_in(stream_key, 6), dim), (shards_of,), jnp.float32, low / len(cuts), top_value / len(cuts))
        loudness = loudness * jnp.repeat(jnp.exp(steps), dims[dim] // shards_of).reshape((-1,) + (1,) * (len(dims) - 1 - dim))
    return loudness


def shared_out(rng, own, number, rows, number_of, top, bound, slope):
    order = jax.random.permutation(rng, number_of)
    crowded, ordinary = load_shares(number_of, rows * top, bound, slope, True), load_shares(number_of, rows * top, bound, slope, False)
    places = jnp.arange(number_of)

    def named(sizes, offset_by):
        used = int((sizes > 0).sum())
        fixed = max(1, used // 4)
        moved = fixed + (places - fixed + offset_by * (used - fixed)) % max(1, number_of - fixed)
        return jnp.zeros((number_of,), jnp.int32).at[order[jnp.where(places < fixed, places, moved)]].set(jnp.asarray(sizes, jnp.int32))

    sizes = jnp.where(number % 4 == 0, named(crowded, number // 4), named(ordinary, number - number // 4 - 1))
    mixed = jax.random.permutation(jax.random.fold_in(own, 3), number_of)
    source_of, sink = mixed[0:number_of // 2 * 2:2], mixed[1:number_of // 2 * 2:2]
    slack = jnp.minimum(sizes[source_of] - 1, bound - sizes[sink]) // 2
    slack = jnp.where((source_of == order[0]) | (sink == order[0]) | (sizes[sink] == 0), 0, jnp.maximum(slack, 0))
    moved = jax.random.randint(jax.random.fold_in(own, 4), (number_of // 2,), 0, 1 << 20) % (slack + 1)
    sizes = sizes.at[source_of].add(-moved).at[sink].add(moved)
    members = jnp.searchsorted(jnp.cumsum(sizes), jnp.arange(rows * top), side="right").astype(jnp.int32)
    listing = members.reshape(top, rows).T
    listing = listing[jax.random.permutation(jax.random.fold_in(own, 1), rows)]
    offset_by = jax.random.randint(jax.random.fold_in(own, 2), (rows, 1), 0, top)
    return jnp.take_along_axis(listing, (jnp.arange(top)[None, :] + offset_by) % top, axis=1)


def load_shares(number_of, total, reach, lean, full):
    weights = [(1 << 20) // math.isqrt(standing ** lean) + 1 for standing in range(1, number_of + 1)]
    largest = reach if full else min(reach, max(-(-total // number_of), total * weights[0] // sum(weights)))
    least = 1 if total - largest >= number_of - 1 else 0
    given, surplus = [largest] + [least] * (number_of - 1), total - largest - least * (number_of - 1)
    while surplus > 0:
        free = [i for i in range(1, number_of) if given[i] < largest] or [i for i in range(1, number_of) if given[i] < reach]
        pool, left = sum([weights[i] for i in free]), surplus
        for i in free:
            addition = min(reach - given[i], max(1, left * weights[i] // pool), surplus)
            given[i] = given[i] + addition
            surplus = surplus - addition
    return np.array(given)


def scatter_about(key, dims, deviation, limit, cuts=(), kind=jnp.bfloat16):
    drawn = jax.random.normal(key, dims, jnp.float32) * deviation
    if len(cuts) > 0:
        drawn = block_scale(key, dims, cuts, -0.22, 0.18) * drawn
    return jnp.clip(drawn, min=-limit, max=limit).astype(kind)


def setup_inputs(seed: int = 0) -> dict:
    arg_keys = jax.random.split(jax.random.key(seed), 9)
    queries = draw_queries(jax.random.fold_in(arg_keys[8], 71), 0)
    resident_cache = scatter_about(arg_keys[1], (SEQUENCE_TOTAL, RESIDENT_PAGES * PAGE_TOKENS, KEY_VALUE_HEADS, KEY_LATENT_RANK + VALUE_LATENT_RANK), 1.0, 6.0, ((0, 8), (2, 4)))
    overflow_cache = scatter_about(arg_keys[2], (N_DP, N_DP, SPILL_CAPACITY, PAGE_TOKENS, KEY_VALUE_HEADS, KEY_LATENT_RANK + VALUE_LATENT_RANK), 1.0, 6.0, ((0, 8), (4, 4)))
    key_up_weight = scatter_about(arg_keys[3], (KEY_VALUE_HEADS, KEY_LATENT_RANK, HEAD_DIMENSION), KEY_LATENT_RANK ** -0.5, 0.75, ((0, 4),))
    value_up_weight = scatter_about(arg_keys[4], (KEY_VALUE_HEADS, VALUE_LATENT_RANK, HEAD_DIMENSION), VALUE_LATENT_RANK ** -0.5, 0.75, ((0, 4),))
    lengths = with_ends(jax.random.randint(arg_keys[5], (SEQUENCE_TOTAL,), RESIDENT_PAGES * PAGE_TOKENS + 1, (RESIDENT_PAGES + REMOTE_PAGES) * PAGE_TOKENS + 1), jax.random.fold_in(arg_keys[5], 1), RESIDENT_PAGES * PAGE_TOKENS + 1, (RESIDENT_PAGES + REMOTE_PAGES) * PAGE_TOKENS).astype(jnp.int32)
    routes_keys = jax.random.split(jax.random.fold_in(arg_keys[6], 1), SEQUENCE_TOTAL * REMOTE_PAGES // (SEQ_DEV * REMOTE_PAGES))
    routes_turns = jax.random.permutation(jax.random.fold_in(arg_keys[6], 3), SEQUENCE_TOTAL * REMOTE_PAGES // (SEQ_DEV * REMOTE_PAGES))
    routes = jax.vmap(lambda own, number: shared_out(jax.random.fold_in(arg_keys[6], 2), own, number, SEQ_DEV * REMOTE_PAGES, N_DP, 1, SPILL_CAPACITY, 2))(routes_keys, routes_turns).reshape((SEQUENCE_TOTAL, REMOTE_PAGES, 1))
    out_weight = scatter_about(arg_keys[7], (QUERY_HEADS * HEAD_DIMENSION, D), (QUERY_HEADS * HEAD_DIMENSION) ** -0.5, 0.0625, ((0, 4), (1, 8)))
    return {"queries": queries, "resident_cache": resident_cache, "overflow_cache": overflow_cache, "key_up_weight": key_up_weight, "value_up_weight": value_up_weight, "lengths": lengths, "routes": routes, "out_weight": out_weight}


def spill_ranks(targets):
    entry_count = targets.shape[-1]
    position = jnp.arange(entry_count, dtype=jnp.int32)
    same_target = targets[..., :, None] == targets[..., None, :]
    earlier = position[None, :] < position[:, None]
    return lax.optimization_barrier(jnp.sum((same_target & earlier).astype(jnp.int32), axis=-1)).astype(jnp.int32)

def reference(queries, resident_cache, overflow_cache, key_up_weight, value_up_weight, lengths, routes, out_weight):
    targets = routes[:, :, 0].reshape(N_DP, SEQ_DEV * REMOTE_PAGES)
    ranking = spill_ranks(targets).reshape(N_DP * SEQ_DEV, REMOTE_PAGES)
    targets = targets.reshape(N_DP * SEQ_DEV, REMOTE_PAGES)
    key_table = key_up_weight.astype(jnp.float32)
    value_table = value_up_weight.astype(jnp.float32)
    head_cluster = QUERY_HEADS // KEY_VALUE_HEADS
    token_total = (RESIDENT_PAGES + REMOTE_PAGES) * PAGE_TOKENS
    score_scale = 1.0 / math.sqrt(HEAD_DIMENSION)

    def one_sequence(packed):
        sequence, single_query, resident_rows, length, target_row, rank_row = packed
        owner_group = (sequence // SEQ_DEV).astype(jnp.int32)
        remote_rows = overflow_cache[target_row, owner_group, rank_row]
        latent_vector = jnp.concatenate([resident_rows, remote_rows.reshape(REMOTE_PAGES * PAGE_TOKENS, KEY_VALUE_HEADS, KEY_LATENT_RANK + VALUE_LATENT_RANK)], axis=0).astype(jnp.float32)
        rebuilt_keys = jnp.einsum('thr,hrd->thd', latent_vector[..., :KEY_LATENT_RANK], key_table)
        rebuilt_values = jnp.einsum('thr,hrd->thd', latent_vector[..., KEY_LATENT_RANK:], value_table)
        group_sorted = single_query.astype(jnp.float32).reshape(KEY_VALUE_HEADS, head_cluster, HEAD_DIMENSION)
        scores = jnp.einsum('hgd,thd->hgt', group_sorted, rebuilt_keys, precision=lax.Precision.HIGHEST) * score_scale
        token_mask = jnp.arange(token_total, dtype=jnp.int32) < length
        scores = jnp.where(token_mask[None, None, :], scores, -jnp.inf)
        probs = jax.nn.softmax(scores, axis=-1)
        weighted = jnp.einsum('hgt,thd->hgd', probs, rebuilt_values, precision=lax.Precision.HIGHEST)
        return weighted.reshape(QUERY_HEADS * HEAD_DIMENSION).astype(jnp.bfloat16)
    sequences = jnp.arange(N_DP * SEQ_DEV, dtype=jnp.int32)
    attended = lax.map(one_sequence, (sequences, queries, resident_cache, lengths, targets, ranking))
    return jnp.dot(attended, out_weight, preferred_element_type=jnp.float32).astype(jnp.bfloat16)
```

```python
import math

import jax
import jax.numpy as jnp
from jax import lax
from jax.experimental import pallas as pl
from jax.experimental.pallas import tpu as pltpu
from jax.sharding import PartitionSpec as P

very_low = -1e30
f32 = jnp.float32
bf16 = jnp.bfloat16
lanes = 128
half = 64
pad_heads = 16
stat_lanes = 16


def three_terms(value):
    high = value.astype(bf16)
    rest = value - high.astype(f32)
    middle = rest.astype(bf16)
    low = (rest - middle.astype(f32)).astype(bf16)
    return high, middle, low


def absorbed_queries(query_rows, key_up, kv_heads):
    scale = math.log2(math.e) / math.sqrt(key_up.shape[1])
    product = lax.dot_general(
        query_rows, key_up, (((1,), (1,)), ((), ())), preferred_element_type=f32
    )
    lane = lax.broadcasted_iota(jnp.int32, (1, 1, lanes), 2)
    if kv_heads == 2:
        product = product.reshape(-1, 2, 8, lanes)
        first = product[:, 0]
        second = pltpu.roll(product[:, 1].reshape(-1, lanes), half, 1).reshape(first.shape)
    else:
        product = jnp.concatenate([product, jnp.zeros_like(product)], axis=1)
        first = product.reshape(-1, 8, lanes)
        second = jnp.zeros_like(first)
    both = jnp.concatenate([first, second], axis=1)
    both = jnp.where(lane < half, both * scale, 0.0)
    return jnp.concatenate(three_terms(both), axis=1)


def attend(query_terms, latent, valid):
    scores = lax.dot_general(
        query_terms, latent, (((1,), (1,)), ((), ())), preferred_element_type=f32
    )
    scores = scores[0:16] + scores[16:32] + scores[32:48]
    scores = jnp.where(valid, scores, very_low)
    peak = jnp.max(scores, axis=1, keepdims=True)
    weights = jnp.exp2(scores - peak)
    total = jnp.sum(weights, axis=1, keepdims=True)
    high = weights.astype(bf16)
    low = (weights - high.astype(f32)).astype(bf16)
    weighted = jnp.dot(
        jnp.concatenate([high, low], axis=0), latent, preferred_element_type=f32
    )
    weighted = (weighted[0:16] + weighted[16:32]) / total
    lane = lax.broadcasted_iota(jnp.int32, (8, lanes), 1)
    packed = jnp.where(lane < half, pltpu.roll(weighted[0:8], half, 1), weighted[8:16])
    return packed, peak + jnp.log2(total)


def row_masks(rows, kv_heads):
    column = lax.broadcasted_iota(jnp.int32, (pad_heads, rows), 1)
    head = lax.broadcasted_iota(jnp.int32, (pad_heads, rows), 0) // 8
    if kv_heads == 1:
        return column, head == 0
    return column // 2, (column % 2) == head


def solution(mesh):
    group_count = mesh.shape["dp"]
    head_parts = mesh.shape["mp"]

    def home_kernel(
        routes, lengths, own, queries, key_up, resident,
        item_sequence, item_tokens, entry_item, entry_ok, packed_out, lse_out,
        table, counts, holder_counts,
    ):
        seq_dev, rows, _ = resident.shape
        kv_heads = key_up.shape[0] // half
        items = item_sequence.shape[0]
        slots = items // group_count
        entry_count = routes.shape[0] // group_count
        tail_pages = entry_count // seq_dev
        home_tokens = rows // kv_heads
        page = lanes
        me = own[0]

        def scan_group(group, _):
            count = jnp.int32(0)
            for entry in range(entry_count):
                table[group * slots + count] = entry
                count = count + (routes[group * entry_count + entry] == me).astype(jnp.int32)
            counts[group] = count
            return 0

        lax.fori_loop(0, group_count, scan_group, 0)

        def finish_item(group, _):
            for slot in range(slots):
                here = slot < counts[group]
                entry = jnp.where(here, table[group * slots + slot], 0)
                row = entry // tail_pages
                sequence = group * seq_dev + row
                first = home_tokens + (entry - row * tail_pages) * page
                count = jnp.clip(lengths[sequence] - first, 0, page)
                item_sequence[group * slots + slot] = sequence
                item_tokens[group * slots + slot] = jnp.where(here, count, 0)
            return 0

        lax.fori_loop(0, group_count, finish_item, 0)

        def clear(holder, _):
            holder_counts[holder] = 0
            return 0

        lax.fori_loop(0, group_count, clear, 0)

        def own_row(row, _):
            length = lengths[me * seq_dev + row]
            for page_index in range(tail_pages):
                entry = row * tail_pages + page_index
                holder = routes[me * entry_count + entry]
                slot = holder_counts[holder]
                holder_counts[holder] = slot + 1
                entry_item[entry] = holder * slots + slot
                entry_ok[entry] = (home_tokens + page_index * page < length).astype(jnp.int32)
            return 0

        lax.fori_loop(0, seq_dev, own_row, 0)

        terms = absorbed_queries(queries[...], key_up[...], kv_heads)
        token, head_ok = row_masks(rows, kv_heads)
        for row in range(seq_dev):
            valid = head_ok & (token < lengths[me * seq_dev + row])
            packed, lse = attend(terms[row], resident[row], valid)
            packed_out[row] = packed
            lse_out[row] = jnp.broadcast_to(lse, (pad_heads, lanes))

    def page_kernel(
        item_sequence, item_tokens, queries, key_up, overflow, out, pages, terms_ref, sems
    ):
        items, rows, _ = overflow.shape
        slots = items // group_count
        kv_heads = key_up.shape[0] // half

        def copy_of(group):
            part = pl.ds(group * slots, slots)
            return pltpu.make_async_copy(overflow.at[part], pages.at[part], sems.at[group])

        for group in range(group_count):
            copy_of(group).start()
        terms_ref[...] = absorbed_queries(queries[...], key_up[...], kv_heads)
        token, head_ok = row_masks(rows, kv_heads)
        stat_lane = lax.broadcasted_iota(jnp.int32, (pad_heads, lanes), 1)

        def one_group(group, _):
            copy_of(group).wait()
            stats = jnp.zeros((pad_heads, lanes), f32)
            for slot in range(slots):
                item = group * slots + slot
                valid = head_ok & (token < item_tokens[item])
                packed, lse = attend(terms_ref[item_sequence[item]], pages[item], valid)
                out[group, slot] = packed.astype(bf16)
                for place, term in enumerate(three_terms(lse)):
                    chosen = stat_lane == slot * stat_lanes + place
                    stats = jnp.where(chosen, term.astype(f32), stats)
            out[group, slots] = stats[0:8].astype(bf16)
            out[group, slots + 1] = stats[8:16].astype(bf16)
            return 0

        lax.fori_loop(0, group_count, one_group, 0)

    def merge_kernel(entry_item, entry_ok, received, packed_home, lse_home, out, rows_ref):
        seq_dev = packed_home.shape[0]
        slots = received.shape[1] - 2
        tail_pages = entry_item.shape[0] // seq_dev
        lane8 = lax.broadcasted_iota(jnp.int32, (8, lanes), 1)
        lane16 = lax.broadcasted_iota(jnp.int32, (pad_heads, lanes), 1)
        is_term = (lane16 % stat_lanes) < 3
        slot_of_lane = lane16 // stat_lanes

        def spread(value):
            return jnp.where(lane8 < half, value[0:8], value[8:16])

        for row in range(seq_dev):
            parts = [(lse_home[row], packed_home[row])]
            for page_index in range(tail_pages):
                entry = row * tail_pages + page_index
                item = entry_item[entry]
                holder = item // slots
                slot = item - holder * slots
                stats = jnp.concatenate(
                    [received[holder, slots].astype(f32), received[holder, slots + 1].astype(f32)],
                    axis=0,
                )
                mine = is_term & (slot_of_lane == slot)
                lse = jnp.sum(jnp.where(mine, stats, 0.0), axis=1, keepdims=True)
                lse = jnp.where(entry_ok[entry] > 0, lse, very_low)
                lse = jnp.broadcast_to(lse, (pad_heads, lanes))
                parts.append((lse, received[holder, slot].astype(f32)))
            peak = parts[0][0]
            for lse, _ in parts[1:]:
                peak = jnp.maximum(peak, lse)
            total = jnp.zeros((8, lanes), f32)
            merged = jnp.zeros((8, lanes), f32)
            for lse, packed in parts:
                factor = spread(jnp.exp2(lse - peak))
                total = total + factor
                merged = merged + factor * packed
            rows_ref[row * 8 : (row + 1) * 8, :] = merged / total
        for query in range(8):
            block = rows_ref[pl.ds(query, seq_dev, stride=8), :].astype(bf16)
            for target in range(group_count):
                out[target, query] = block

    def project_kernel(received, value_up, weight, out):
        sequences = received.shape[0] * received.shape[2]
        kv_heads = value_up.shape[1] // lanes
        pieces = [
            jnp.dot(
                received[:, query].astype(f32).reshape(sequences, lanes).astype(bf16),
                value_up[...],
                preferred_element_type=f32,
            ).astype(bf16)
            for query in range(8)
        ]
        attended = jnp.concatenate(
            [
                piece[:, head * lanes : (head + 1) * lanes]
                for head in range(kv_heads)
                for piece in pieces
            ],
            axis=1,
        )
        result = jnp.dot(attended, weight[...], preferred_element_type=f32)
        out[...] = result.astype(bf16)

    def body(
        queries, resident_cache, overflow_cache, key_up_weight, value_up_weight,
        lengths, routes, out_weight,
    ):
        seq_dev, head_dev, head_size = queries.shape
        kv_heads, width, _ = key_up_weight.shape
        slots = overflow_cache.shape[2]
        page = overflow_cache.shape[3]
        items = group_count * slots
        tail_pages = routes.shape[1]
        home_tokens = resident_cache.shape[1]
        smem = pl.BlockSpec(memory_space=pltpu.SMEM)
        vmem = pl.BlockSpec(memory_space=pltpu.VMEM)
        hbm = pl.BlockSpec(memory_space=pl.ANY)
        ints = lambda size: jax.ShapeDtypeStruct((size,), jnp.int32)
        own = lax.axis_index("dp").astype(jnp.int32).reshape(1)
        flat_routes = routes.reshape(-1)
        key_up = key_up_weight.reshape(kv_heads * width, head_size)
        flat_queries = queries.reshape(seq_dev * head_dev, head_size)

        spread_queries = jnp.broadcast_to(
            flat_queries[None], (group_count,) + flat_queries.shape
        )
        all_queries = lax.all_to_all(
            spread_queries, "dp", split_axis=0, concat_axis=0, tiled=True
        ).reshape(-1, head_size)

        entries = seq_dev * tail_pages
        item_sequence, item_tokens, entry_item, entry_ok, packed_home, lse_home = pl.pallas_call(
            home_kernel,
            out_shape=(
                ints(items), ints(items), ints(entries), ints(entries),
                jax.ShapeDtypeStruct((seq_dev, 8, lanes), f32),
                jax.ShapeDtypeStruct((seq_dev, pad_heads, lanes), f32),
            ),
            in_specs=[smem, smem, smem, vmem, vmem, vmem],
            out_specs=(smem, smem, smem, smem, vmem, vmem),
            scratch_shapes=[
                pltpu.SMEM((items + 8,), jnp.int32),
                pltpu.SMEM((group_count,), jnp.int32),
                pltpu.SMEM((group_count,), jnp.int32),
            ],
            cost_estimate=pl.CostEstimate(
                flops=200_000_000, transcendentals=0, bytes_accessed=1 << 20
            ),
        )(
            flat_routes, lengths, own, flat_queries, key_up,
            resident_cache.reshape(seq_dev, home_tokens * kv_heads, lanes),
        )

        partials = pl.pallas_call(
            page_kernel,
            out_shape=jax.ShapeDtypeStruct((group_count, slots + 2, 8, lanes), bf16),
            in_specs=[smem, smem, vmem, vmem, hbm],
            out_specs=vmem,
            scratch_shapes=[
                pltpu.VMEM((items, page * kv_heads, lanes), bf16),
                pltpu.VMEM((group_count * seq_dev, 48, lanes), bf16),
                pltpu.SemaphoreType.DMA((group_count,)),
            ],
        )(
            item_sequence, item_tokens, all_queries, key_up,
            overflow_cache.reshape(items, page * kv_heads, lanes),
        )
        partials = lax.all_to_all(partials, "dp", split_axis=0, concat_axis=0, tiled=True)

        merged = pl.pallas_call(
            merge_kernel,
            out_shape=jax.ShapeDtypeStruct((group_count, 8, seq_dev, lanes), bf16),
            in_specs=[smem, smem, vmem, vmem, vmem],
            out_specs=vmem,
            scratch_shapes=[pltpu.VMEM((seq_dev * 8, lanes), f32)],
        )(entry_item, entry_ok, partials, packed_home, lse_home)
        merged = lax.all_to_all(merged, "dp", split_axis=0, concat_axis=0, tiled=True)

        blocks = jnp.eye(kv_heads, dtype=bf16)[:, None, :, None] * value_up_weight[:, :, None, :]
        blocks = blocks.reshape(kv_heads * width, kv_heads * head_size)
        blocks = jnp.pad(blocks, ((0, lanes - kv_heads * width), (0, 0)))
        sequences = group_count * seq_dev
        partial_out = pl.pallas_call(
            project_kernel,
            out_shape=jax.ShapeDtypeStruct((sequences, out_weight.shape[1]), bf16),
            in_specs=[vmem, vmem, vmem],
            out_specs=vmem,
        )(merged, blocks, out_weight)
        pieces = lax.all_to_all(
            partial_out.reshape(head_parts, sequences // head_parts, -1),
            "mp", split_axis=0, concat_axis=0, tiled=True,
        )
        return jnp.sum(pieces.astype(f32), axis=0).astype(bf16)

    placed = (
        P("dp", "mp", None),
        P("dp", None, "mp", None),
        P("dp", None, None, None, "mp", None),
        P("mp", None, None),
        P("mp", None, None),
        P(),
        P(),
        P("mp", "dp"),
    )
    return jax.shard_map(body, mesh=mesh, in_specs=placed, out_specs=P("mp", "dp"), check_vma=False)
```

```python
import math

import jax
import jax.numpy as jnp
from jax import lax
from jax.experimental import pallas as pl
from jax.experimental.pallas import tpu as pltpu
from jax.sharding import PartitionSpec as P

very_low = -1e30
f32 = jnp.float32
bf16 = jnp.bfloat16
lanes = 128
half = 64
pad_heads = 16
stat_lanes = 16
batch = 8


def three_terms(value):
    high = value.astype(bf16)
    rest = value - high.astype(f32)
    middle = rest.astype(bf16)
    low = (rest - middle.astype(f32)).astype(bf16)
    return high, middle, low


def absorbed_queries(query_rows, key_up, kv_heads):
    scale = math.log2(math.e) / math.sqrt(key_up.shape[1])
    product = lax.dot_general(
        query_rows, key_up, (((1,), (1,)), ((), ())), preferred_element_type=f32
    )
    lane = lax.broadcasted_iota(jnp.int32, (1, 1, lanes), 2)
    if kv_heads == 2:
        product = product.reshape(-1, 2, 8, lanes)
        first = product[:, 0]
        second = pltpu.roll(product[:, 1].reshape(-1, lanes), half, 1).reshape(first.shape)
    else:
        product = jnp.concatenate([product, jnp.zeros_like(product)], axis=1)
        first = product.reshape(-1, 8, lanes)
        second = jnp.zeros_like(first)
    both = jnp.concatenate([first, second], axis=1)
    both = jnp.where(lane < half, both * scale, 0.0)
    return jnp.concatenate(three_terms(both), axis=1)


def attend_all(query_terms, latents, valid):
    products = [
        lax.dot_general(terms, latent, (((1,), (1,)), ((), ())), preferred_element_type=f32)
        for terms, latent in zip(query_terms, latents)
    ]
    scores = [
        jnp.where(ok, product[0:16] + product[16:32] + product[32:48], very_low)
        for ok, product in zip(valid, products)
    ]
    peaks = [jnp.max(score, axis=1, keepdims=True) for score in scores]
    weights = [jnp.exp2(score - peak) for score, peak in zip(scores, peaks)]
    split = []
    for weight in weights:
        high = weight.astype(bf16)
        low = (weight - high.astype(f32)).astype(bf16)
        split.append(jnp.concatenate([high, low], axis=0))
    sums = [
        jnp.dot(terms, latent, preferred_element_type=f32)
        for terms, latent in zip(split, latents)
    ]
    totals = [jnp.sum(weight, axis=1, keepdims=True) for weight in weights]
    lane = lax.broadcasted_iota(jnp.int32, (8, lanes), 1)
    packed = []
    for weighted, total in zip(sums, totals):
        weighted = (weighted[0:16] + weighted[16:32]) / total
        packed.append(
            jnp.where(lane < half, pltpu.roll(weighted[0:8], half, 1), weighted[8:16])
        )
    return packed, [peak + jnp.log2(total) for peak, total in zip(peaks, totals)]


def row_masks(rows, kv_heads):
    column = lax.broadcasted_iota(jnp.int32, (pad_heads, rows), 1)
    head = lax.broadcasted_iota(jnp.int32, (pad_heads, rows), 0) // 8
    if kv_heads == 1:
        return column, head == 0
    return column // 2, (column % 2) == head


def pin(array):
    return pltpu.with_memory_space_constraint(array, pltpu.VMEM)


def near(shape, kind):
    return pltpu.VMEM(shape, kind)


def solution(mesh):
    group_count = mesh.shape["dp"]
    head_parts = mesh.shape["mp"]

    def home_kernel(
        routes, lengths, own, queries, key_up, resident,
        item_sequence, item_tokens, item_list, item_count, entry_item, entry_ok,
        packed_out, lse_out, table, counts, holder_counts,
    ):
        seq_dev, rows, _ = resident.shape
        kv_heads = key_up.shape[0] // half
        items = item_sequence.shape[0]
        slots = items // group_count
        tail_pages = routes.shape[0]
        home_tokens = rows // kv_heads
        page = lanes
        me = own[0]

        def scan_group(group, _):
            count = jnp.int32(0)
            for row in range(seq_dev):
                for place in range(tail_pages):
                    table[group * slots + count] = row * tail_pages + place
                    named = routes[place, group * seq_dev + row] == me
                    count = count + named.astype(jnp.int32)
            counts[group] = count
            holder_counts[group] = 0
            return 0

        lax.fori_loop(0, group_count, scan_group, 0)

        def finish_group(group, found):
            for slot in range(slots):
                item = group * slots + slot
                here = slot < counts[group]
                entry = jnp.where(here, table[item], 0)
                row = entry // tail_pages
                sequence = group * seq_dev + row
                first = home_tokens + (entry - row * tail_pages) * page
                tokens = jnp.where(here, jnp.clip(lengths[sequence] - first, 0, page), 0)
                item_sequence[item] = sequence
                item_tokens[item] = tokens
                item_list[found] = item
                found = found + (tokens > 0).astype(jnp.int32)
            return found

        item_count[0] = lax.fori_loop(0, group_count, finish_group, jnp.int32(0))

        def own_row(row, _):
            length = lengths[me * seq_dev + row]
            for place in range(tail_pages):
                entry = row * tail_pages + place
                holder = routes[place, me * seq_dev + row]
                slot = holder_counts[holder]
                holder_counts[holder] = slot + 1
                entry_item[entry] = holder * slots + slot
                entry_ok[entry] = (home_tokens + place * page < length).astype(jnp.int32)
            return 0

        lax.fori_loop(0, seq_dev, own_row, 0)

        terms = absorbed_queries(queries[...], key_up[...], kv_heads)
        token, head_ok = row_masks(rows, kv_heads)
        for start in range(0, seq_dev, 4):
            part = range(start, min(start + 4, seq_dev))
            packed, lse = attend_all(
                [terms[row] for row in part],
                [resident[row] for row in part],
                [head_ok & (token < lengths[me * seq_dev + row]) for row in part],
            )
            for place, row in enumerate(part):
                packed_out[row] = packed[place]
                lse_out[row] = jnp.broadcast_to(lse[place], (pad_heads, lanes))

    def page_kernel(
        item_sequence, item_tokens, item_list, item_count, queries, key_up, overflow,
        out, pages, terms_ref, stats_ref, sems,
    ):
        items, rows, _ = overflow.shape
        slots = items // group_count
        kv_heads = key_up.shape[0] // half
        found = item_count[0]

        def copy_of(place):
            return pltpu.make_async_copy(
                overflow.at[item_list[place]], pages.at[place], sems.at[place]
            )

        def start_copy(place, _):
            copy_of(place).start()
            return 0

        lax.fori_loop(0, found, start_copy, 0)
        terms_ref[...] = absorbed_queries(queries[...], key_up[...], kv_heads)
        token, head_ok = row_masks(rows, kv_heads)
        stat_lane = lax.broadcasted_iota(jnp.int32, (pad_heads, lanes), 1)

        def one_batch(step, _):
            first = step * batch
            for offset in range(batch):
                @pl.when(first + offset < found)
                def _():
                    copy_of(first + offset).wait()

            places = [jnp.minimum(first + offset, found - 1) for offset in range(batch)]
            chosen = [item_list[place] for place in places]
            packed, lse = attend_all(
                [terms_ref[item_sequence[item]] for item in chosen],
                [pages[place] for place in places],
                [head_ok & (token < item_tokens[item]) for item in chosen],
            )
            for offset, item in enumerate(chosen):
                group = item // slots
                slot = item - group * slots
                out[group, slot] = packed[offset].astype(bf16)
                stats = stats_ref[group]
                for place, term in enumerate(three_terms(lse[offset])):
                    mine = stat_lane == slot * stat_lanes + place
                    stats = jnp.where(mine, term.astype(f32), stats)
                stats_ref[group] = stats
            return 0

        lax.fori_loop(0, (found + batch - 1) // batch, one_batch, 0)
        out[:, slots] = stats_ref[:, 0:8].astype(bf16)
        out[:, slots + 1] = stats_ref[:, 8:16].astype(bf16)

    def merge_kernel(entry_item, entry_ok, received, packed_home, lse_home, out, rows_ref):
        seq_dev = packed_home.shape[0]
        slots = received.shape[1] - 2
        tail_pages = entry_item.shape[0] // seq_dev
        lane8 = lax.broadcasted_iota(jnp.int32, (8, lanes), 1)
        lane16 = lax.broadcasted_iota(jnp.int32, (pad_heads, lanes), 1)
        is_term = (lane16 % stat_lanes) < 3
        slot_of_lane = lane16 // stat_lanes

        def spread(value):
            return jnp.where(lane8 < half, value[0:8], value[8:16])

        for row in range(seq_dev):
            parts = [(lse_home[row], packed_home[row])]
            for page_index in range(tail_pages):
                entry = row * tail_pages + page_index
                item = entry_item[entry]
                holder = item // slots
                slot = item - holder * slots
                stats = jnp.concatenate(
                    [received[holder, slots].astype(f32), received[holder, slots + 1].astype(f32)],
                    axis=0,
                )
                mine = is_term & (slot_of_lane == slot)
                lse = jnp.sum(jnp.where(mine, stats, 0.0), axis=1, keepdims=True)
                lse = jnp.where(entry_ok[entry] > 0, lse, very_low)
                lse = jnp.broadcast_to(lse, (pad_heads, lanes))
                packed = jnp.where(entry_ok[entry] > 0, received[holder, slot].astype(f32), 0.0)
                parts.append((lse, packed))
            peak = parts[0][0]
            for lse, _ in parts[1:]:
                peak = jnp.maximum(peak, lse)
            total = jnp.zeros((8, lanes), f32)
            merged = jnp.zeros((8, lanes), f32)
            for lse, packed in parts:
                factor = spread(jnp.exp2(lse - peak))
                total = total + factor
                merged = merged + factor * packed
            rows_ref[row * 8 : (row + 1) * 8, :] = merged / total
        for query in range(8):
            block = rows_ref[pl.ds(query, seq_dev, stride=8), :].astype(bf16)
            for target in range(group_count):
                out[target, query] = block

    def project_kernel(received, value_up, weight, out):
        sequences = received.shape[0] * received.shape[2]
        kv_heads = value_up.shape[1] // lanes
        pieces = [
            jnp.dot(
                received[:, query].astype(f32).reshape(sequences, lanes).astype(bf16),
                value_up[...],
                preferred_element_type=f32,
            )
            for query in range(8)
        ]
        attended = jnp.concatenate(
            [
                piece[:, head * lanes : (head + 1) * lanes]
                for head in range(kv_heads)
                for piece in pieces
            ],
            axis=1,
        )
        high = attended.astype(bf16)
        low = (attended - high.astype(f32)).astype(bf16)
        both = jnp.concatenate([high, low], axis=0)
        result = jnp.dot(both, weight[...], preferred_element_type=f32)
        out[...] = (result[:sequences] + result[sequences:]).astype(bf16)

    def body(
        queries, resident_cache, overflow_cache, key_up_weight, value_up_weight,
        lengths, routes, out_weight,
    ):
        seq_dev, head_dev, head_size = queries.shape
        kv_heads, width, _ = key_up_weight.shape
        slots = overflow_cache.shape[2]
        page = overflow_cache.shape[3]
        items = group_count * slots
        tail_pages = routes.shape[1]
        home_tokens = resident_cache.shape[1]
        smem = pl.BlockSpec(memory_space=pltpu.SMEM)
        vmem = pl.BlockSpec(memory_space=pltpu.VMEM)
        hbm = pl.BlockSpec(memory_space=pl.ANY)
        ints = lambda size: jax.ShapeDtypeStruct((size,), jnp.int32)
        own = lax.axis_index("dp").astype(jnp.int32).reshape(1)
        flat_routes = routes[:, :, 0].T
        key_up = key_up_weight.reshape(kv_heads * width, head_size)
        flat_queries = queries.reshape(seq_dev * head_dev, head_size)

        spread_queries = jnp.broadcast_to(
            flat_queries[None], (group_count,) + flat_queries.shape
        )
        all_queries = lax.all_to_all(
            spread_queries, "dp", split_axis=0, concat_axis=0, tiled=True
        ).reshape(-1, head_size)

        entries = seq_dev * tail_pages
        (
            item_sequence, item_tokens, item_list, item_count, entry_item, entry_ok,
            packed_home, lse_home,
        ) = pl.pallas_call(
            home_kernel,
            out_shape=(
                ints(items), ints(items), ints(items), ints(1), ints(entries), ints(entries),
                near((seq_dev, 8, lanes), f32),
                near((seq_dev, pad_heads, lanes), f32),
            ),
            in_specs=[smem, smem, smem, vmem, vmem, vmem],
            out_specs=(smem, smem, smem, smem, smem, smem, vmem, vmem),
            scratch_shapes=[
                pltpu.SMEM((items + 8,), jnp.int32),
                pltpu.SMEM((group_count,), jnp.int32),
                pltpu.SMEM((group_count,), jnp.int32),
            ],
            cost_estimate=pl.CostEstimate(
                flops=200_000_000, transcendentals=0, bytes_accessed=1 << 20
            ),
        )(
            flat_routes, lengths, own, flat_queries, key_up,
            resident_cache.reshape(seq_dev, home_tokens * kv_heads, lanes),
        )

        partials = pl.pallas_call(
            page_kernel,
            out_shape=near((group_count, slots + 2, 8, lanes), bf16),
            in_specs=[smem, smem, smem, smem, vmem, vmem, hbm],
            out_specs=vmem,
            scratch_shapes=[
                pltpu.VMEM((items, page * kv_heads, lanes), bf16),
                pltpu.VMEM((group_count * seq_dev, 48, lanes), bf16),
                pltpu.VMEM((group_count, pad_heads, lanes), f32),
                pltpu.SemaphoreType.DMA((items,)),
            ],
        )(
            item_sequence, item_tokens, item_list, item_count, pin(all_queries), key_up,
            overflow_cache.reshape(items, page * kv_heads, lanes),
        )
        partials = lax.all_to_all(partials, "dp", split_axis=0, concat_axis=0, tiled=True)

        merged = pl.pallas_call(
            merge_kernel,
            out_shape=near((group_count, 8, seq_dev, lanes), bf16),
            in_specs=[smem, smem, vmem, vmem, vmem],
            out_specs=vmem,
            scratch_shapes=[pltpu.VMEM((seq_dev * 8, lanes), f32)],
        )(entry_item, entry_ok, pin(partials), pin(packed_home), pin(lse_home))
        merged = lax.all_to_all(merged, "dp", split_axis=0, concat_axis=0, tiled=True)

        blocks = jnp.eye(kv_heads, dtype=bf16)[:, None, :, None] * value_up_weight[:, :, None, :]
        blocks = blocks.reshape(kv_heads * width, kv_heads * head_size)
        blocks = jnp.pad(blocks, ((0, lanes - kv_heads * width), (0, 0)))
        sequences = group_count * seq_dev
        partial_out = pl.pallas_call(
            project_kernel,
            out_shape=near((sequences, out_weight.shape[1]), bf16),
            in_specs=[vmem, vmem, vmem],
            out_specs=vmem,
        )(pin(merged), blocks, out_weight)
        pieces = lax.all_to_all(
            partial_out.reshape(head_parts, sequences // head_parts, -1),
            "mp", split_axis=0, concat_axis=0, tiled=True,
        )
        return jnp.sum(pieces.astype(f32), axis=0).astype(bf16)

    placed = (
        P("dp", "mp", None),
        P("dp", None, "mp", None),
        P("dp", None, None, None, "mp", None),
        P("mp", None, None),
        P("mp", None, None),
        P(),
        P(),
        P("mp", "dp"),
    )
    return jax.shard_map(body, mesh=mesh, in_specs=placed, out_specs=P("mp", "dp"), check_vma=False)
```

```python
import math

import jax
import jax.numpy as jnp
from jax import lax
from jax.experimental import pallas as pl
from jax.experimental.pallas import tpu as pltpu
from jax.sharding import PartitionSpec as P

very_low = -1e30
f32 = jnp.float32
bf16 = jnp.bfloat16
lanes = 128
half = 64
pad_heads = 16
stat_lanes = 16
batch = 8


def three_terms(value):
    high = value.astype(bf16)
    rest = value - high.astype(f32)
    middle = rest.astype(bf16)
    low = (rest - middle.astype(f32)).astype(bf16)
    return high, middle, low


def absorbed_queries(query_rows, key_up, kv_heads):
    scale = math.log2(math.e) / math.sqrt(key_up.shape[1])
    product = lax.dot_general(
        query_rows, key_up, (((1,), (1,)), ((), ())), preferred_element_type=f32
    )
    lane = lax.broadcasted_iota(jnp.int32, (1, 1, lanes), 2)
    if kv_heads == 2:
        product = product.reshape(-1, 2, 8, lanes)
        first = product[:, 0]
        second = pltpu.roll(product[:, 1].reshape(-1, lanes), half, 1).reshape(first.shape)
    else:
        product = jnp.concatenate([product, jnp.zeros_like(product)], axis=1)
        first = product.reshape(-1, 8, lanes)
        second = jnp.zeros_like(first)
    both = jnp.concatenate([first, second], axis=1)
    both = jnp.where(lane < half, both * scale, 0.0)
    return jnp.concatenate(three_terms(both), axis=1)


def attend_all(query_terms, latents, valid):
    products = [
        lax.dot_general(terms, latent, (((1,), (1,)), ((), ())), preferred_element_type=f32)
        for terms, latent in zip(query_terms, latents)
    ]
    scores = [
        jnp.where(ok, product[0:16] + product[16:32] + product[32:48], very_low)
        for ok, product in zip(valid, products)
    ]
    peaks = [jnp.max(score, axis=1, keepdims=True) for score in scores]
    weights = [jnp.exp2(score - peak) for score, peak in zip(scores, peaks)]
    split = []
    for weight in weights:
        high = weight.astype(bf16)
        low = (weight - high.astype(f32)).astype(bf16)
        split.append(jnp.concatenate([high, low], axis=0))
    sums = [
        jnp.dot(terms, latent, preferred_element_type=f32)
        for terms, latent in zip(split, latents)
    ]
    totals = [jnp.sum(weight, axis=1, keepdims=True) for weight in weights]
    lane = lax.broadcasted_iota(jnp.int32, (8, lanes), 1)
    packed = []
    for weighted, total in zip(sums, totals):
        weighted = (weighted[0:16] + weighted[16:32]) / total
        packed.append(
            jnp.where(lane < half, pltpu.roll(weighted[0:8], half, 1), weighted[8:16])
        )
    return packed, [peak + jnp.log2(total) for peak, total in zip(peaks, totals)]


def row_masks(rows, kv_heads):
    column = lax.broadcasted_iota(jnp.int32, (pad_heads, rows), 1)
    head = lax.broadcasted_iota(jnp.int32, (pad_heads, rows), 0) // 8
    if kv_heads == 1:
        return column, head == 0
    return column // 2, (column % 2) == head


def pin(array):
    return pltpu.with_memory_space_constraint(array, pltpu.VMEM)


def far(array):
    return pltpu.with_memory_space_constraint(array, pltpu.HBM)


def near(shape, kind):
    return pltpu.VMEM(shape, kind)


def solution(mesh):
    group_count = mesh.shape["dp"]
    head_parts = mesh.shape["mp"]

    def home_kernel(
        routes, lengths, own, queries, key_up, value_up, resident_far,
        item_sequence, item_tokens, item_list, item_count, entry_item, entry_ok,
        packed_out, lse_out, blocks, key_near,
        table, counts, holder_counts, resident, home_sem,
    ):
        seq_dev, rows, _ = resident.shape
        home_copy = pltpu.make_async_copy(resident_far, resident, home_sem)
        home_copy.start()
        kv_heads = key_up.shape[0] // half
        items = item_sequence.shape[0]
        slots = items // group_count
        tail_pages = routes.shape[0]
        home_tokens = rows // kv_heads
        page = lanes
        me = own[0]

        def scan_group(group, _):
            count = jnp.int32(0)
            for row in range(seq_dev):
                for place in range(tail_pages):
                    table[group * slots + count] = row * tail_pages + place
                    named = routes[place, 0, group * seq_dev + row] == me
                    count = count + named.astype(jnp.int32)
            counts[group] = count
            holder_counts[group] = 0
            return 0

        lax.fori_loop(0, group_count, scan_group, 0)

        def finish_group(group, found):
            for slot in range(slots):
                item = group * slots + slot
                here = slot < counts[group]
                entry = jnp.where(here, table[item], 0)
                row = entry // tail_pages
                sequence = group * seq_dev + row
                first = home_tokens + (entry - row * tail_pages) * page
                tokens = jnp.where(here, jnp.clip(lengths[sequence] - first, 0, page), 0)
                item_sequence[item] = sequence
                item_tokens[item] = tokens
                item_list[found] = item
                found = found + (tokens > 0).astype(jnp.int32)
            return found

        item_count[0] = lax.fori_loop(0, group_count, finish_group, jnp.int32(0))

        def own_row(row, _):
            length = lengths[me * seq_dev + row]
            for place in range(tail_pages):
                entry = row * tail_pages + place
                holder = routes[place, 0, me * seq_dev + row]
                slot = holder_counts[holder]
                holder_counts[holder] = slot + 1
                entry_item[entry] = holder * slots + slot
                entry_ok[entry] = (home_tokens + place * page < length).astype(jnp.int32)
            return 0

        lax.fori_loop(0, seq_dev, own_row, 0)

        key_near[...] = key_up[...]
        blocks[...] = jnp.zeros(blocks.shape, bf16)
        for head in range(kv_heads):
            across = slice(head * lanes, (head + 1) * lanes)
            blocks[head * half : (head + 1) * half, across] = value_up[head]
        terms = absorbed_queries(queries[...], key_up[...], kv_heads)
        token, head_ok = row_masks(rows, kv_heads)
        home_copy.wait()
        for start in range(0, seq_dev, 4):
            part = range(start, min(start + 4, seq_dev))
            packed, lse = attend_all(
                [terms[row] for row in part],
                [resident[row] for row in part],
                [head_ok & (token < lengths[me * seq_dev + row]) for row in part],
            )
            for place, row in enumerate(part):
                packed_out[row] = packed[place]
                lse_out[row] = jnp.broadcast_to(lse[place], (pad_heads, lanes))

    def page_kernel(
        item_sequence, item_tokens, item_list, item_count, queries, key_up, overflow,
        out, pages, terms_ref, stats_ref, sems,
    ):
        items, rows, _ = overflow.shape
        slots = items // group_count
        kv_heads = key_up.shape[0] // half
        found = item_count[0]

        def copy_of(place):
            return pltpu.make_async_copy(
                overflow.at[item_list[place]], pages.at[place], sems.at[place]
            )

        def start_copy(place, _):
            copy_of(place).start()
            return 0

        lax.fori_loop(0, found, start_copy, 0)
        terms_ref[...] = absorbed_queries(queries[...], key_up[...], kv_heads)
        token, head_ok = row_masks(rows, kv_heads)
        stat_lane = lax.broadcasted_iota(jnp.int32, (pad_heads, lanes), 1)

        def one_batch(step, _):
            first = step * batch
            for offset in range(batch):
                @pl.when(first + offset < found)
                def _():
                    copy_of(first + offset).wait()

            places = [jnp.minimum(first + offset, found - 1) for offset in range(batch)]
            chosen = [item_list[place] for place in places]
            packed, lse = attend_all(
                [terms_ref[item_sequence[item]] for item in chosen],
                [pages[place] for place in places],
                [head_ok & (token < item_tokens[item]) for item in chosen],
            )
            for offset, item in enumerate(chosen):
                group = item // slots
                slot = item - group * slots
                out[group, slot] = packed[offset].astype(bf16)
                stats = stats_ref[group]
                for place, term in enumerate(three_terms(lse[offset])):
                    mine = stat_lane == slot * stat_lanes + place
                    stats = jnp.where(mine, term.astype(f32), stats)
                stats_ref[group] = stats
            return 0

        lax.fori_loop(0, (found + batch - 1) // batch, one_batch, 0)
        out[:, slots] = stats_ref[:, 0:8].astype(bf16)
        out[:, slots + 1] = stats_ref[:, 8:16].astype(bf16)

    def merge_kernel(entry_item, entry_ok, received, packed_home, lse_home, out, rows_ref):
        seq_dev = packed_home.shape[0]
        slots = received.shape[1] - 2
        tail_pages = entry_item.shape[0] // seq_dev
        lane8 = lax.broadcasted_iota(jnp.int32, (8, lanes), 1)
        lane16 = lax.broadcasted_iota(jnp.int32, (pad_heads, lanes), 1)
        is_term = (lane16 % stat_lanes) < 3
        slot_of_lane = lane16 // stat_lanes

        def spread(value):
            return jnp.where(lane8 < half, value[0:8], value[8:16])

        for row in range(seq_dev):
            parts = [(lse_home[row], packed_home[row])]
            for page_index in range(tail_pages):
                entry = row * tail_pages + page_index
                item = entry_item[entry]
                holder = item // slots
                slot = item - holder * slots
                stats = jnp.concatenate(
                    [received[holder, slots].astype(f32), received[holder, slots + 1].astype(f32)],
                    axis=0,
                )
                mine = is_term & (slot_of_lane == slot)
                lse = jnp.sum(jnp.where(mine, stats, 0.0), axis=1, keepdims=True)
                lse = jnp.where(entry_ok[entry] > 0, lse, very_low)
                lse = jnp.broadcast_to(lse, (pad_heads, lanes))
                packed = jnp.where(entry_ok[entry] > 0, received[holder, slot].astype(f32), 0.0)
                parts.append((lse, packed))
            peak = parts[0][0]
            for lse, _ in parts[1:]:
                peak = jnp.maximum(peak, lse)
            total = jnp.zeros((8, lanes), f32)
            merged = jnp.zeros((8, lanes), f32)
            for lse, packed in parts:
                factor = spread(jnp.exp2(lse - peak))
                total = total + factor
                merged = merged + factor * packed
            rows_ref[row * 8 : (row + 1) * 8, :] = merged / total
        for query in range(8):
            block = rows_ref[pl.ds(query, seq_dev, stride=8), :].astype(bf16)
            for target in range(group_count):
                out[target, query] = block

    def project_kernel(own, received, value_up, weight, *rest):
        outs, out = rest[:head_parts], rest[head_parts]
        sequences = received.shape[0] * received.shape[2]
        kv_heads = value_up.shape[1] // lanes
        pieces = [
            jnp.dot(
                received[:, query].astype(f32).reshape(sequences, lanes).astype(bf16),
                value_up[...],
                preferred_element_type=f32,
            )
            for query in range(8)
        ]
        attended = jnp.concatenate(
            [
                piece[:, head * lanes : (head + 1) * lanes]
                for head in range(kv_heads)
                for piece in pieces
            ],
            axis=1,
        )
        high = attended.astype(bf16)
        low = (attended - high.astype(f32)).astype(bf16)
        both = jnp.concatenate([high, low], axis=0)
        result = jnp.dot(both, weight[...], preferred_element_type=f32)
        out[...] = (result[:sequences] + result[sequences:]).astype(bf16).reshape(out.shape)
        for step in range(head_parts):
            outs[step][...] = out[(own[1] + step) % head_parts]

    def body(
        queries, resident_cache, overflow_cache, key_up_weight, value_up_weight,
        lengths, routes, out_weight,
    ):
        seq_dev, head_dev, head_size = queries.shape
        kv_heads, width, _ = key_up_weight.shape
        slots = overflow_cache.shape[2]
        page = overflow_cache.shape[3]
        items = group_count * slots
        tail_pages = routes.shape[1]
        home_tokens = resident_cache.shape[1]
        smem = pl.BlockSpec(memory_space=pltpu.SMEM)
        vmem = pl.BlockSpec(memory_space=pltpu.VMEM)
        hbm = pl.BlockSpec(memory_space=pltpu.HBM)
        small = pltpu.CompilerParams(vmem_limit_bytes=16 << 20)
        ints = lambda size: jax.ShapeDtypeStruct((size,), jnp.int32)
        own = jnp.stack([lax.axis_index("dp"), lax.axis_index("mp")]).astype(jnp.int32)
        flat_routes = routes.transpose(1, 2, 0)
        key_up = key_up_weight.reshape(kv_heads * width, head_size)
        flat_queries = queries.reshape(seq_dev * head_dev, head_size)

        spread_queries = jnp.broadcast_to(
            flat_queries[None], (group_count,) + flat_queries.shape
        )
        all_queries = lax.all_to_all(
            spread_queries, "dp", split_axis=0, concat_axis=0, tiled=True
        ).reshape(-1, head_size)

        entries = seq_dev * tail_pages
        (
            item_sequence, item_tokens, item_list, item_count, entry_item, entry_ok,
            packed_home, lse_home, blocks, key_near,
        ) = pl.pallas_call(
            home_kernel,
            out_shape=(
                ints(items), ints(items), ints(items), ints(1), ints(entries), ints(entries),
                near((seq_dev, 8, lanes), f32),
                near((seq_dev, pad_heads, lanes), f32),
                near((lanes, kv_heads * head_size), bf16),
                near(key_up.shape, bf16),
            ),
            in_specs=[smem, smem, smem, vmem, vmem, vmem, hbm],
            out_specs=(smem,) * 6 + (vmem,) * 4,
            scratch_shapes=[
                pltpu.SMEM((items + 8,), jnp.int32),
                pltpu.SMEM((group_count,), jnp.int32),
                pltpu.SMEM((group_count,), jnp.int32),
                pltpu.VMEM((seq_dev, home_tokens * kv_heads, lanes), bf16),
                pltpu.SemaphoreType.DMA,
            ],
            cost_estimate=pl.CostEstimate(
                flops=200_000_000, transcendentals=0, bytes_accessed=1 << 20
            ),
        )(
            flat_routes, lengths, own, flat_queries, key_up, value_up_weight,
            resident_cache.reshape(seq_dev, home_tokens * kv_heads, lanes),
        )

        partials = pl.pallas_call(
            page_kernel,
            out_shape=near((group_count, slots + 2, 8, lanes), bf16),
            in_specs=[smem, smem, smem, smem, vmem, vmem, hbm],
            out_specs=vmem,
            scratch_shapes=[
                pltpu.VMEM((items, page * kv_heads, lanes), bf16),
                pltpu.VMEM((group_count * seq_dev, 48, lanes), bf16),
                pltpu.VMEM((group_count, pad_heads, lanes), f32),
                pltpu.SemaphoreType.DMA((items,)),
            ],
            compiler_params=small,
        )(
            item_sequence, item_tokens, item_list, item_count, pin(all_queries), pin(key_near),
            far(overflow_cache.reshape(items, page * kv_heads, lanes)),
        )
        partials = lax.all_to_all(partials, "dp", split_axis=0, concat_axis=0, tiled=True)

        merged = pl.pallas_call(
            merge_kernel,
            out_shape=near((group_count, 8, seq_dev, lanes), bf16),
            in_specs=[smem, smem, vmem, vmem, vmem],
            out_specs=vmem,
            scratch_shapes=[pltpu.VMEM((seq_dev * 8, lanes), f32)],
            compiler_params=small,
        )(entry_item, entry_ok, pin(partials), pin(packed_home), pin(lse_home))
        merged = lax.all_to_all(merged, "dp", split_axis=0, concat_axis=0, tiled=True)

        sequences = group_count * seq_dev
        width_out = out_weight.shape[1]
        piece = (sequences // head_parts, width_out)
        pieces = pl.pallas_call(
            project_kernel,
            out_shape=(near(piece, bf16),) * head_parts,
            in_specs=[smem, vmem, vmem, vmem],
            out_specs=(vmem,) * head_parts,
            scratch_shapes=[
                pltpu.VMEM((head_parts,) + piece, bf16),
            ],
            compiler_params=small,
        )(own, pin(merged), pin(blocks), out_weight)
        total = pieces[0].astype(f32)
        for step in range(1, head_parts):
            ring = [(source, (source + step) % head_parts) for source in range(head_parts)]
            total = total + lax.ppermute(pieces[step], "mp", ring).astype(f32)
        return total.astype(bf16)

    placed = (
        P("dp", "mp", None),
        P("dp", None, "mp", None),
        P("dp", None, None, None, "mp", None),
        P("mp", None, None),
        P("mp", None, None),
        P(),
        P(),
        P("mp", "dp"),
    )
    return jax.shard_map(body, mesh=mesh, in_specs=placed, out_specs=P("mp", "dp"), check_vma=False)
```

```python
import math

import jax
import jax.numpy as jnp
from jax import lax
from jax.experimental import pallas as pl
from jax.experimental.pallas import tpu as pltpu
from jax.sharding import PartitionSpec as P

very_low = -1e30
f32 = jnp.float32
bf16 = jnp.bfloat16
lanes = 128
half = 64
pad_heads = 16
stat_lanes = 16
batch = 8
early_bytes = 5 << 19


def three_terms(value):
    high = value.astype(bf16)
    rest = value - high.astype(f32)
    middle = rest.astype(bf16)
    low = (rest - middle.astype(f32)).astype(bf16)
    return high, middle, low


def absorbed_queries(query_rows, key_up, kv_heads):
    scale = math.log2(math.e) / math.sqrt(key_up.shape[1])
    product = lax.dot_general(
        query_rows, key_up, (((1,), (1,)), ((), ())), preferred_element_type=f32
    )
    lane = lax.broadcasted_iota(jnp.int32, (1, 1, lanes), 2)
    if kv_heads == 2:
        product = product.reshape(-1, 2, 8, lanes)
        first = product[:, 0]
        second = pltpu.roll(product[:, 1].reshape(-1, lanes), half, 1).reshape(first.shape)
    else:
        product = jnp.concatenate([product, jnp.zeros_like(product)], axis=1)
        first = product.reshape(-1, 8, lanes)
        second = jnp.zeros_like(first)
    both = jnp.concatenate([first, second], axis=1)
    both = jnp.where(lane < half, both * scale, 0.0)
    return jnp.concatenate(three_terms(both), axis=1)


def attend_all(query_terms, latents, valid):
    products = [
        lax.dot_general(terms, latent, (((1,), (1,)), ((), ())), preferred_element_type=f32)
        for terms, latent in zip(query_terms, latents)
    ]
    scores = [
        jnp.where(ok, product[0:16] + product[16:32] + product[32:48], very_low)
        for ok, product in zip(valid, products)
    ]
    peaks = [jnp.max(score, axis=1, keepdims=True) for score in scores]
    weights = [jnp.exp2(score - peak) for score, peak in zip(scores, peaks)]
    split = []
    for weight in weights:
        high = weight.astype(bf16)
        low = (weight - high.astype(f32)).astype(bf16)
        split.append(jnp.concatenate([high, low], axis=0))
    sums = [
        jnp.dot(terms, latent, preferred_element_type=f32)
        for terms, latent in zip(split, latents)
    ]
    totals = [jnp.sum(weight, axis=1, keepdims=True) for weight in weights]
    lane = lax.broadcasted_iota(jnp.int32, (8, lanes), 1)
    packed = []
    for weighted, total in zip(sums, totals):
        weighted = (weighted[0:16] + weighted[16:32]) / total
        packed.append(
            jnp.where(lane < half, pltpu.roll(weighted[0:8], half, 1), weighted[8:16])
        )
    return packed, [peak + jnp.log2(total) for peak, total in zip(peaks, totals)]


def row_masks(rows, kv_heads):
    column = lax.broadcasted_iota(jnp.int32, (pad_heads, rows), 1)
    head = lax.broadcasted_iota(jnp.int32, (pad_heads, rows), 0) // 8
    if kv_heads == 1:
        return column, head == 0
    return column // 2, (column % 2) == head


def pin(array):
    return pltpu.with_memory_space_constraint(array, pltpu.VMEM)


def table_of(array):
    return pltpu.with_memory_space_constraint(array, pltpu.SMEM)


def far(array):
    return pltpu.with_memory_space_constraint(array, pltpu.HBM)


def near(shape, kind):
    return pltpu.VMEM(shape, kind)


def solution(mesh):
    group_count = mesh.shape["dp"]
    head_parts = mesh.shape["mp"]

    def home_kernel(
        routes, lengths, queries, key_up, value_up, resident_far, overflow,
        item_sequence, item_tokens, item_list, item_count, entry_item, entry_ok,
        packed_out, lse_out, blocks, key_near, pages,
        table, counts, holder_counts, resident, home_sem, sems,
    ):
        seq_dev, rows, _ = resident.shape
        home_copy = pltpu.make_async_copy(resident_far, resident, home_sem)
        home_copy.start()
        kv_heads = key_up.shape[0] // half
        items = item_sequence.shape[0]
        slots = items // group_count
        tail_pages = routes.shape[0]
        home_tokens = rows // kv_heads
        page = lanes
        me = lax.axis_index("dp")

        def scan_group(group, _):
            count = jnp.int32(0)
            for row in range(seq_dev):
                for place in range(tail_pages):
                    table[group * slots + count] = row * tail_pages + place
                    named = routes[place, 0, group * seq_dev + row] == me
                    count = count + named.astype(jnp.int32)
            counts[group] = count
            holder_counts[group] = 0
            return 0

        lax.fori_loop(0, group_count, scan_group, 0)

        def finish_group(group, found):
            for slot in range(slots):
                item = group * slots + slot
                here = slot < counts[group]
                entry = jnp.where(here, table[item], 0)
                row = entry // tail_pages
                sequence = group * seq_dev + row
                first = home_tokens + (entry - row * tail_pages) * page
                tokens = jnp.where(here, jnp.clip(lengths[sequence] - first, 0, page), 0)
                item_sequence[item] = sequence
                item_tokens[item] = tokens
                item_list[found] = item
                found = found + (tokens > 0).astype(jnp.int32)
            return found

        found_count = lax.fori_loop(0, group_count, finish_group, jnp.int32(0))
        item_count[0] = found_count

        def page_copy(place):
            return pltpu.make_async_copy(
                overflow.at[item_list[place]], pages.at[place], sems.at[place]
            )

        def start_copy(place, _):
            page_copy(place).start()
            return 0

        def end_copy(place, _):
            page_copy(place).wait()
            return 0

        early_count = jnp.minimum(found_count, pages.shape[0])
        lax.fori_loop(0, early_count, start_copy, 0)

        def own_row(row, _):
            length = lengths[me * seq_dev + row]
            for place in range(tail_pages):
                entry = row * tail_pages + place
                holder = routes[place, 0, me * seq_dev + row]
                slot = holder_counts[holder]
                holder_counts[holder] = slot + 1
                entry_item[entry] = holder * slots + slot
                entry_ok[entry] = (home_tokens + place * page < length).astype(jnp.int32)
            return 0

        lax.fori_loop(0, seq_dev, own_row, 0)

        key_near[...] = key_up[...]
        blocks[...] = jnp.zeros(blocks.shape, bf16)
        for head in range(kv_heads):
            across = slice(head * lanes, (head + 1) * lanes)
            blocks[head * half : (head + 1) * half, across] = value_up[head]
        terms = absorbed_queries(queries[...], key_up[...], kv_heads)
        token, head_ok = row_masks(rows, kv_heads)
        home_copy.wait()
        for start in range(0, seq_dev, 4):
            part = range(start, min(start + 4, seq_dev))
            packed, lse = attend_all(
                [terms[row] for row in part],
                [resident[row] for row in part],
                [head_ok & (token < lengths[me * seq_dev + row]) for row in part],
            )
            for place, row in enumerate(part):
                packed_out[row] = packed[place]
                lse_out[row] = jnp.broadcast_to(lse[place], (pad_heads, lanes))
        lax.fori_loop(0, early_count, end_copy, 0)

    def page_kernel(
        item_sequence, item_tokens, item_list, item_count, queries, key_up, pages, overflow,
        out, terms_ref, stats_ref, *late,
    ):
        early, rows, _ = pages.shape
        items = overflow.shape[0]
        slots = items // group_count
        kv_heads = key_up.shape[0] // half
        found = item_count[0]

        def late_copy(place):
            late_pages, sems = late
            return pltpu.make_async_copy(
                overflow.at[item_list[place]], late_pages.at[place - early], sems.at[place - early]
            )

        def start_copy(place, _):
            late_copy(place).start()
            return 0

        if late:
            lax.fori_loop(early, found, start_copy, 0)
        terms_ref[...] = absorbed_queries(queries[...], key_up[...], kv_heads)
        token, head_ok = row_masks(rows, kv_heads)
        stat_lane = lax.broadcasted_iota(jnp.int32, (pad_heads, lanes), 1)

        def one_batch(step, source, shift):
            first = step * batch
            places = [jnp.minimum(first + offset, found - 1) for offset in range(batch)]
            chosen = [item_list[place] for place in places]
            packed, lse = attend_all(
                [terms_ref[item_sequence[item]] for item in chosen],
                [source[place - shift] for place in places],
                [head_ok & (token < item_tokens[item]) for item in chosen],
            )
            for offset, item in enumerate(chosen):
                group = item // slots
                slot = item - group * slots
                out[group, slot] = packed[offset].astype(bf16)
                stats = stats_ref[group]
                for place, term in enumerate(three_terms(lse[offset])):
                    mine = stat_lane == slot * stat_lanes + place
                    stats = jnp.where(mine, term.astype(f32), stats)
                stats_ref[group] = stats

        def early_batch(step, _):
            one_batch(step, pages, 0)
            return 0

        def late_batch(step, _):
            for offset in range(batch):
                @pl.when(step * batch + offset < found)
                def _():
                    late_copy(step * batch + offset).wait()

            one_batch(step, late[0], early)
            return 0

        steps = (found + batch - 1) // batch
        lax.fori_loop(0, jnp.minimum(steps, early // batch), early_batch, 0)
        if late:
            lax.fori_loop(early // batch, steps, late_batch, 0)
        out[:, slots] = stats_ref[:, 0:8].astype(bf16)
        out[:, slots + 1] = stats_ref[:, 8:16].astype(bf16)

    def merge_kernel(entry_item, entry_ok, received, packed_home, lse_home, out, rows_ref):
        seq_dev = packed_home.shape[0]
        slots = received.shape[1] - 2
        tail_pages = entry_item.shape[0] // seq_dev
        lane8 = lax.broadcasted_iota(jnp.int32, (8, lanes), 1)
        lane16 = lax.broadcasted_iota(jnp.int32, (pad_heads, lanes), 1)
        is_term = (lane16 % stat_lanes) < 3
        slot_of_lane = lane16 // stat_lanes

        def spread(value):
            return jnp.where(lane8 < half, value[0:8], value[8:16])

        for row in range(seq_dev):
            parts = [(lse_home[row], packed_home[row])]
            for page_index in range(tail_pages):
                entry = row * tail_pages + page_index
                item = entry_item[entry]
                holder = item // slots
                slot = item - holder * slots
                stats = jnp.concatenate(
                    [received[holder, slots].astype(f32), received[holder, slots + 1].astype(f32)],
                    axis=0,
                )
                mine = is_term & (slot_of_lane == slot)
                lse = jnp.sum(jnp.where(mine, stats, 0.0), axis=1, keepdims=True)
                lse = jnp.where(entry_ok[entry] > 0, lse, very_low)
                lse = jnp.broadcast_to(lse, (pad_heads, lanes))
                packed = jnp.where(entry_ok[entry] > 0, received[holder, slot].astype(f32), 0.0)
                parts.append((lse, packed))
            peak = parts[0][0]
            for lse, _ in parts[1:]:
                peak = jnp.maximum(peak, lse)
            total = jnp.zeros((8, lanes), f32)
            merged = jnp.zeros((8, lanes), f32)
            for lse, packed in parts:
                factor = spread(jnp.exp2(lse - peak))
                total = total + factor
                merged = merged + factor * packed
            rows_ref[row * 8 : (row + 1) * 8, :] = merged / total
        for query in range(8):
            block = rows_ref[pl.ds(query, seq_dev, stride=8), :].astype(bf16)
            for target in range(group_count):
                out[target, query] = block

    def project_kernel(received, value_up, weight, *rest):
        outs, out = rest[:head_parts], rest[head_parts]
        me = lax.axis_index("mp")
        sequences = received.shape[0] * received.shape[2]
        kv_heads = value_up.shape[1] // lanes
        pieces = [
            jnp.dot(
                received[:, query].astype(f32).reshape(sequences, lanes).astype(bf16),
                value_up[...],
                preferred_element_type=f32,
            )
            for query in range(8)
        ]
        attended = jnp.concatenate(
            [
                piece[:, head * lanes : (head + 1) * lanes]
                for head in range(kv_heads)
                for piece in pieces
            ],
            axis=1,
        )
        high = attended.astype(bf16)
        low = (attended - high.astype(f32)).astype(bf16)
        both = jnp.concatenate([high, low], axis=0)
        result = jnp.dot(both, weight[...], preferred_element_type=f32)
        out[...] = (result[:sequences] + result[sequences:]).astype(bf16).reshape(out.shape)
        for step in range(head_parts):
            outs[step][...] = out[(me + step) % head_parts]

    def body(
        queries, resident_cache, overflow_cache, key_up_weight, value_up_weight,
        lengths, routes, out_weight,
    ):
        seq_dev, head_dev, head_size = queries.shape
        kv_heads, width, _ = key_up_weight.shape
        slots = overflow_cache.shape[2]
        page = overflow_cache.shape[3]
        items = group_count * slots
        tail_pages = routes.shape[1]
        home_tokens = resident_cache.shape[1]
        smem = pl.BlockSpec(memory_space=pltpu.SMEM)
        vmem = pl.BlockSpec(memory_space=pltpu.VMEM)
        hbm = pl.BlockSpec(memory_space=pltpu.HBM)
        small = pltpu.CompilerParams(vmem_limit_bytes=16 << 20)
        ints = lambda size: pltpu.SMEM((size,), jnp.int32)
        flat_routes = routes.transpose(1, 2, 0)
        key_up = key_up_weight.reshape(kv_heads * width, head_size)
        flat_queries = queries.reshape(seq_dev * head_dev, head_size)

        spread_queries = jnp.broadcast_to(
            flat_queries[None], (group_count,) + flat_queries.shape
        )
        all_queries = lax.all_to_all(
            spread_queries, "dp", split_axis=0, concat_axis=0, tiled=True
        ).reshape(-1, head_size)

        entries = seq_dev * tail_pages
        early = early_bytes // (page * kv_heads * lanes * 2) // batch * batch
        early = min(-(-items // batch) * batch, early)
        (
            item_sequence, item_tokens, item_list, item_count, entry_item, entry_ok,
            packed_home, lse_home, blocks, key_near, pages,
        ) = pl.pallas_call(
            home_kernel,
            out_shape=(
                ints(items), ints(items), ints(items), ints(1), ints(entries), ints(entries),
                near((seq_dev, 8, lanes), f32),
                near((seq_dev, pad_heads, lanes), f32),
                near((lanes, kv_heads * head_size), bf16),
                near(key_up.shape, bf16),
                near((early, page * kv_heads, lanes), bf16),
            ),
            in_specs=[smem, smem, vmem, vmem, vmem, hbm, hbm],
            out_specs=(smem,) * 6 + (vmem,) * 5,
            scratch_shapes=[
                pltpu.SMEM((items + 8,), jnp.int32),
                pltpu.SMEM((group_count,), jnp.int32),
                pltpu.SMEM((group_count,), jnp.int32),
                pltpu.VMEM((seq_dev, home_tokens * kv_heads, lanes), bf16),
                pltpu.SemaphoreType.DMA,
                pltpu.SemaphoreType.DMA((early,)),
            ],
            compiler_params=small,
            cost_estimate=pl.CostEstimate(
                flops=200_000_000, transcendentals=0, bytes_accessed=1 << 20
            ),
        )(
            far(flat_routes), far(lengths), far(flat_queries), far(key_up),
            far(value_up_weight),
            far(resident_cache.reshape(seq_dev, home_tokens * kv_heads, lanes)),
            far(overflow_cache.reshape(items, page * kv_heads, lanes)),
        )

        late = items - early
        late_scratch = [] if late <= 0 else [
            pltpu.VMEM((late, page * kv_heads, lanes), bf16),
            pltpu.SemaphoreType.DMA((late,)),
        ]
        partials = pl.pallas_call(
            page_kernel,
            out_shape=near((group_count, slots + 2, 8, lanes), bf16),
            in_specs=[smem, smem, smem, smem, vmem, vmem, vmem, hbm],
            out_specs=vmem,
            scratch_shapes=[
                pltpu.VMEM((group_count * seq_dev, 48, lanes), bf16),
                pltpu.VMEM((group_count, pad_heads, lanes), f32),
            ] + late_scratch,
            compiler_params=small,
        )(
            table_of(item_sequence), table_of(item_tokens), table_of(item_list),
            table_of(item_count), pin(all_queries), pin(key_near),
            pin(pages), far(overflow_cache.reshape(items, page * kv_heads, lanes)),
        )
        partials = lax.all_to_all(partials, "dp", split_axis=0, concat_axis=0, tiled=True)

        merged = pl.pallas_call(
            merge_kernel,
            out_shape=near((group_count, 8, seq_dev, lanes), bf16),
            in_specs=[smem, smem, vmem, vmem, vmem],
            out_specs=vmem,
            scratch_shapes=[pltpu.VMEM((seq_dev * 8, lanes), f32)],
            compiler_params=small,
        )(table_of(entry_item), table_of(entry_ok), pin(partials), pin(packed_home), pin(lse_home))
        merged = lax.all_to_all(merged, "dp", split_axis=0, concat_axis=0, tiled=True)

        sequences = group_count * seq_dev
        width_out = out_weight.shape[1]
        piece = (sequences // head_parts, width_out)
        pieces = pl.pallas_call(
            project_kernel,
            out_shape=(near(piece, bf16),) * head_parts,
            in_specs=[vmem, vmem, vmem],
            out_specs=(vmem,) * head_parts,
            scratch_shapes=[
                pltpu.VMEM((head_parts,) + piece, bf16),
            ],
            compiler_params=small,
        )(pin(merged), pin(blocks), out_weight)
        total = pieces[0].astype(f32)
        for step in range(1, head_parts):
            ring = [(source, (source + step) % head_parts) for source in range(head_parts)]
            total = total + lax.ppermute(pieces[step], "mp", ring).astype(f32)
        return total.astype(bf16)

    placed = (
        P("dp", "mp", None),
        P("dp", None, "mp", None),
        P("dp", None, None, None, "mp", None),
        P("mp", None, None),
        P("mp", None, None),
        P(),
        P(),
        P("mp", "dp"),
    )
    return jax.shard_map(body, mesh=mesh, in_specs=placed, out_specs=P("mp", "dp"), check_vma=False)
```

```python
import math

import jax
import jax.numpy as jnp
from jax import lax
from jax.experimental import pallas as pl
from jax.experimental.pallas import tpu as pltpu
from jax.sharding import PartitionSpec as P

very_low = -1e30
f32 = jnp.float32
bf16 = jnp.bfloat16
lanes = 128
half = 64
pad_heads = 16
stat_lanes = 16
batch = 24
early_bytes = 3 << 20


def three_terms(value):
    high = value.astype(bf16)
    rest = value - high.astype(f32)
    middle = rest.astype(bf16)
    low = (rest - middle.astype(f32)).astype(bf16)
    return high, middle, low


def absorbed_queries(query_rows, key_up, kv_heads):
    scale = math.log2(math.e) / math.sqrt(key_up.shape[1])
    product = lax.dot_general(
        query_rows, key_up, (((1,), (1,)), ((), ())), preferred_element_type=f32
    )
    lane = lax.broadcasted_iota(jnp.int32, (1, 1, lanes), 2)
    if kv_heads == 2:
        product = product.reshape(-1, 2, 8, lanes)
        first = product[:, 0]
        second = pltpu.roll(product[:, 1].reshape(-1, lanes), half, 1).reshape(first.shape)
    else:
        product = jnp.concatenate([product, jnp.zeros_like(product)], axis=1)
        first = product.reshape(-1, 8, lanes)
        second = jnp.zeros_like(first)
    both = jnp.concatenate([first, second], axis=1)
    both = jnp.where(lane < half, both * scale, 0.0)
    return jnp.concatenate(three_terms(both), axis=1)


def attend_all(query_terms, latents, valid):
    pairs = range(0, len(latents), 2)
    rows = query_terms[0].shape[0]
    beside = [jnp.concatenate([latents[at], latents[at + 1]], axis=1) for at in pairs]
    scores = []
    for at, latent in zip(pairs, beside):
        none = jnp.zeros_like(query_terms[at])
        terms = jnp.concatenate(
            [
                jnp.concatenate([query_terms[at], none], axis=1),
                jnp.concatenate([none, query_terms[at + 1]], axis=1),
            ],
            axis=0,
        )
        product = lax.dot_general(
            terms, latent, (((1,), (1,)), ((), ())), preferred_element_type=f32
        )
        for one, ok in ((product[:rows], valid[at]), (product[rows:], valid[at + 1])):
            scores.append(jnp.where(ok, one[0:16] + one[16:32] + one[32:48], very_low))
    peaks = [jnp.max(score, axis=1, keepdims=True) for score in scores]
    weights = [jnp.exp2(score - peak) for score, peak in zip(scores, peaks)]
    split = []
    for weight in weights:
        high = weight.astype(bf16)
        low = (weight - high.astype(f32)).astype(bf16)
        split += [high, low]
    sums = []
    for at, latent in zip(pairs, beside):
        both = jnp.dot(
            jnp.concatenate(split[2 * at : 2 * at + 4], axis=0), latent,
            preferred_element_type=f32,
        )
        sums += [both[:32, :lanes], both[32:, lanes:]]
    totals = [jnp.sum(weight, axis=1, keepdims=True) for weight in weights]
    lane = lax.broadcasted_iota(jnp.int32, (8, lanes), 1)
    packed = []
    for weighted, total in zip(sums, totals):
        weighted = (weighted[0:16] + weighted[16:32]) / total
        packed.append(
            jnp.where(lane < half, pltpu.roll(weighted[0:8], half, 1), weighted[8:16])
        )
    return packed, [peak + jnp.log2(total) for peak, total in zip(peaks, totals)]


def spread(value):
    lane = lax.broadcasted_iota(jnp.int32, (8, lanes), 1)
    return jnp.where(lane < half, value[0:8], value[8:16])


def row_masks(rows, kv_heads):
    column = lax.broadcasted_iota(jnp.int32, (pad_heads, rows), 1)
    head = lax.broadcasted_iota(jnp.int32, (pad_heads, rows), 0) // 8
    if kv_heads == 1:
        return column, head == 0
    return column // 2, (column % 2) == head


def pin(array):
    return pltpu.with_memory_space_constraint(array, pltpu.VMEM)


def table_of(array):
    return pltpu.with_memory_space_constraint(array, pltpu.SMEM)


def far(array):
    return pltpu.with_memory_space_constraint(array, pltpu.HBM)


def near(shape, kind):
    return pltpu.VMEM(shape, kind)


def solution(mesh):
    group_count = mesh.shape["dp"]
    head_parts = mesh.shape["mp"]

    def partner(source, step):
        paired = head_parts & (head_parts - 1) == 0
        return source ^ step if paired else (source + step) % head_parts

    def home_kernel(
        routes, lengths, queries, key_up, value_up, resident_far, overflow,
        item_sequence, item_tokens, item_list, item_count, entry_item, entry_ok,
        packed_out, lse_out, blocks, key_near, pages,
        table, counts, holder_counts, resident, home_sem, sems,
    ):
        seq_dev, rows, _ = resident.shape
        home_copy = pltpu.make_async_copy(resident_far, resident, home_sem)
        home_copy.start()
        kv_heads = key_up.shape[0] // half
        items = item_sequence.shape[0]
        slots = items // group_count
        tail_pages = routes.shape[0]
        home_tokens = rows // kv_heads
        page = lanes
        me = lax.axis_index("dp")

        def scan_group(group, _):
            count = jnp.int32(0)
            for row in range(seq_dev):
                for place in range(tail_pages):
                    table[group * slots + count] = row * tail_pages + place
                    named = routes[place, 0, group * seq_dev + row] == me
                    count = count + named.astype(jnp.int32)
            counts[group] = count
            holder_counts[group] = 0
            return 0

        lax.fori_loop(0, group_count, scan_group, 0)

        def finish_group(group, found):
            for slot in range(slots):
                item = group * slots + slot
                here = slot < counts[group]
                entry = jnp.where(here, table[item], 0)
                row = entry // tail_pages
                sequence = group * seq_dev + row
                first = home_tokens + (entry - row * tail_pages) * page
                tokens = jnp.where(here, jnp.clip(lengths[sequence] - first, 0, page), 0)
                item_sequence[item] = sequence
                item_tokens[item] = tokens
                item_list[found] = item
                found = found + (tokens > 0).astype(jnp.int32)
            return found

        found_count = lax.fori_loop(0, group_count, finish_group, jnp.int32(0))
        item_count[0] = found_count

        def page_copy(place):
            return pltpu.make_async_copy(
                overflow.at[item_list[place]], pages.at[place], sems.at[place]
            )

        def start_copy(place, _):
            page_copy(place).start()
            return 0

        def end_copy(place, _):
            page_copy(place).wait()
            return 0

        early_count = jnp.minimum(found_count, pages.shape[0])
        lax.fori_loop(0, early_count, start_copy, 0)

        def own_row(row, _):
            length = lengths[me * seq_dev + row]
            for place in range(tail_pages):
                entry = row * tail_pages + place
                holder = routes[place, 0, me * seq_dev + row]
                slot = holder_counts[holder]
                holder_counts[holder] = slot + 1
                entry_item[entry] = holder * slots + slot
                entry_ok[entry] = (home_tokens + place * page < length).astype(jnp.int32)
            return 0

        lax.fori_loop(0, seq_dev, own_row, 0)

        key_near[...] = key_up[...]
        blocks[...] = jnp.zeros(blocks.shape, bf16)
        for head in range(kv_heads):
            across = slice(head * lanes, (head + 1) * lanes)
            blocks[head * half : (head + 1) * half, across] = value_up[head]
        terms = absorbed_queries(queries[...], key_up[...], kv_heads)
        token, head_ok = row_masks(rows, kv_heads)
        home_copy.wait()
        for start in range(0, seq_dev, 4):
            part = range(start, min(start + 4, seq_dev))
            packed, lse = attend_all(
                [terms[row] for row in part],
                [resident[row] for row in part],
                [head_ok & (token < lengths[me * seq_dev + row]) for row in part],
            )
            for place, row in enumerate(part):
                packed_out[row] = packed[place]
                lse_out[row] = spread(lse[place])
        lax.fori_loop(0, early_count, end_copy, 0)

    def page_kernel(
        item_sequence, item_tokens, item_list, item_count, queries, key_up, pages, overflow,
        out, terms_ref, stats_ref, *late,
    ):
        early, rows, _ = pages.shape
        items = overflow.shape[0]
        slots = items // group_count
        kv_heads = key_up.shape[0] // half
        found = item_count[0]

        def late_copy(place):
            late_pages, sems = late
            return pltpu.make_async_copy(
                overflow.at[item_list[place]], late_pages.at[place - early], sems.at[place - early]
            )

        def start_copy(place, _):
            late_copy(place).start()
            return 0

        if late:
            lax.fori_loop(early, found, start_copy, 0)
        terms_ref[...] = absorbed_queries(queries[...], key_up[...], kv_heads)
        token, head_ok = row_masks(rows, kv_heads)
        stat_lane = lax.broadcasted_iota(jnp.int32, (pad_heads, lanes), 1)
        stat_head = lax.broadcasted_iota(jnp.int32, (pad_heads, lanes), 0) // 8
        stat_lane = stat_lane - stat_head * (stat_lanes // 2)

        def one_batch(step, source, shift):
            first = step * batch
            places = [jnp.minimum(first + offset, found - 1) for offset in range(batch)]
            chosen = [item_list[place] for place in places]
            packed, lse = attend_all(
                [terms_ref[item_sequence[item]] for item in chosen],
                [source[place - shift] for place in places],
                [head_ok & (token < item_tokens[item]) for item in chosen],
            )
            for offset, item in enumerate(chosen):
                group = item // slots
                slot = item - group * slots
                out[group, slot] = packed[offset].astype(bf16)
                stats = stats_ref[group]
                for place, term in enumerate(three_terms(lse[offset])):
                    mine = stat_lane == slot * stat_lanes + place
                    stats = jnp.where(mine, term.astype(f32), stats)
                stats_ref[group] = stats

        def early_batch(step, _):
            one_batch(step, pages, 0)
            return 0

        def late_batch(step, _):
            for offset in range(batch):
                @pl.when(step * batch + offset < found)
                def _():
                    late_copy(step * batch + offset).wait()

            one_batch(step, late[0], early)
            return 0

        steps = (found + batch - 1) // batch
        lax.fori_loop(0, jnp.minimum(steps, early // batch), early_batch, 0)
        if late:
            lax.fori_loop(early // batch, steps, late_batch, 0)
        lane = lax.broadcasted_iota(jnp.int32, (group_count, 8, lanes), 2)
        stats = jnp.where(
            lane % stat_lanes < stat_lanes // 2, stats_ref[:, 0:8], stats_ref[:, 8:16]
        )
        out[:, slots] = stats.astype(bf16)

    def merge_kernel(entry_item, entry_ok, received, packed_home, lse_home, out, rows_ref):
        seq_dev = packed_home.shape[0]
        slots = received.shape[1] - 1
        tail_pages = entry_item.shape[0] // seq_dev
        lane = lax.broadcasted_iota(jnp.int32, (8, lanes), 1)
        place = lane % stat_lanes
        slot_of_lane = lane // stat_lanes
        for row in range(seq_dev):
            parts = [(lse_home[row], packed_home[row])]
            for page_index in range(tail_pages):
                entry = row * tail_pages + page_index
                item = entry_item[entry]
                holder = item // slots
                slot = item - holder * slots
                stats = jnp.where(slot_of_lane == slot, received[holder, slots].astype(f32), 0.0)
                pair = [
                    jnp.sum(
                        jnp.where((place >= start) & (place < start + 3), stats, 0.0),
                        axis=1, keepdims=True,
                    )
                    for start in (0, stat_lanes // 2)
                ]
                ok = entry_ok[entry] > 0
                lse = jnp.where(ok, jnp.where(lane < half, pair[0], pair[1]), very_low)
                packed = jnp.where(ok, received[holder, slot].astype(f32), 0.0)
                parts.append((lse, packed))
            peak = parts[0][0]
            for lse, _ in parts[1:]:
                peak = jnp.maximum(peak, lse)
            total = jnp.zeros((8, lanes), f32)
            merged = jnp.zeros((8, lanes), f32)
            for lse, packed in parts:
                factor = jnp.exp2(lse - peak)
                total = total + factor
                merged = merged + factor * packed
            rows_ref[row * 8 : (row + 1) * 8, :] = merged / total
        for query in range(8):
            block = rows_ref[pl.ds(query, seq_dev, stride=8), :].astype(bf16)
            for target in range(group_count):
                out[target, query] = block

    def project_kernel(received, value_up, weight, *rest):
        outs, out = rest[:head_parts], rest[head_parts]
        me = lax.axis_index("mp")
        sequences = received.shape[0] * received.shape[2]
        kv_heads = value_up.shape[1] // lanes
        pieces = [
            jnp.dot(
                received[:, query].astype(f32).reshape(sequences, lanes).astype(bf16),
                value_up[...],
                preferred_element_type=f32,
            )
            for query in range(8)
        ]
        attended = jnp.concatenate(
            [
                piece[:, head * lanes : (head + 1) * lanes]
                for head in range(kv_heads)
                for piece in pieces
            ],
            axis=1,
        )
        high = attended.astype(bf16)
        low = (attended - high.astype(f32)).astype(bf16)
        both = jnp.concatenate([high, low], axis=0)
        result = jnp.dot(both, weight[...], preferred_element_type=f32)
        out[...] = (result[:sequences] + result[sequences:]).astype(bf16).reshape(out.shape)
        for step in range(head_parts):
            outs[step][...] = out[partner(me, step)]

    def body(
        queries, resident_cache, overflow_cache, key_up_weight, value_up_weight,
        lengths, routes, out_weight,
    ):
        seq_dev, head_dev, head_size = queries.shape
        kv_heads, width, _ = key_up_weight.shape
        slots = overflow_cache.shape[2]
        page = overflow_cache.shape[3]
        items = group_count * slots
        tail_pages = routes.shape[1]
        home_tokens = resident_cache.shape[1]
        smem = pl.BlockSpec(memory_space=pltpu.SMEM)
        vmem = pl.BlockSpec(memory_space=pltpu.VMEM)
        hbm = pl.BlockSpec(memory_space=pltpu.HBM)
        small = pltpu.CompilerParams(vmem_limit_bytes=16 << 20)
        ints = lambda size: pltpu.SMEM((size,), jnp.int32)
        flat_routes = routes.transpose(1, 2, 0)
        key_up = key_up_weight.reshape(kv_heads * width, head_size)
        flat_queries = queries.reshape(seq_dev * head_dev, head_size)

        spread_queries = jnp.broadcast_to(
            flat_queries[None], (group_count,) + flat_queries.shape
        )
        all_queries = lax.all_to_all(
            spread_queries, "dp", split_axis=0, concat_axis=0, tiled=True
        ).reshape(-1, head_size)

        entries = seq_dev * tail_pages
        early = early_bytes // (page * kv_heads * lanes * 2) // batch * batch
        early = min(-(-items // batch) * batch, early)
        (
            item_sequence, item_tokens, item_list, item_count, entry_item, entry_ok,
            packed_home, lse_home, blocks, key_near, pages,
        ) = pl.pallas_call(
            home_kernel,
            out_shape=(
                ints(items), ints(items), ints(items), ints(1), ints(entries), ints(entries),
                near((seq_dev, 8, lanes), f32),
                near((seq_dev, 8, lanes), f32),
                near((lanes, kv_heads * head_size), bf16),
                near(key_up.shape, bf16),
                near((early, page * kv_heads, lanes), bf16),
            ),
            in_specs=[smem, smem, vmem, vmem, vmem, hbm, hbm],
            out_specs=(smem,) * 6 + (vmem,) * 5,
            scratch_shapes=[
                pltpu.SMEM((items + 8,), jnp.int32),
                pltpu.SMEM((group_count,), jnp.int32),
                pltpu.SMEM((group_count,), jnp.int32),
                pltpu.VMEM((seq_dev, home_tokens * kv_heads, lanes), bf16),
                pltpu.SemaphoreType.DMA,
                pltpu.SemaphoreType.DMA((early,)),
            ],
            compiler_params=small,
            cost_estimate=pl.CostEstimate(
                flops=200_000_000, transcendentals=0, bytes_accessed=1 << 20
            ),
        )(
            far(flat_routes), far(lengths), far(flat_queries), far(key_up),
            far(value_up_weight),
            far(resident_cache.reshape(seq_dev, home_tokens * kv_heads, lanes)),
            far(overflow_cache.reshape(items, page * kv_heads, lanes)),
        )

        late = items - early
        late_scratch = [] if late <= 0 else [
            pltpu.VMEM((late, page * kv_heads, lanes), bf16),
            pltpu.SemaphoreType.DMA((late,)),
        ]
        partials = pl.pallas_call(
            page_kernel,
            out_shape=near((group_count, slots + 1, 8, lanes), bf16),
            in_specs=[smem, smem, smem, smem, vmem, vmem, vmem, hbm],
            out_specs=vmem,
            scratch_shapes=[
                pltpu.VMEM((group_count * seq_dev, 48, lanes), bf16),
                pltpu.VMEM((group_count, pad_heads, lanes), f32),
            ] + late_scratch,
            compiler_params=small,
        )(
            table_of(item_sequence), table_of(item_tokens), table_of(item_list),
            table_of(item_count), pin(all_queries), pin(key_near),
            pin(pages), far(overflow_cache.reshape(items, page * kv_heads, lanes)),
        )
        partials = lax.all_to_all(partials, "dp", split_axis=0, concat_axis=0, tiled=True)

        merged = pl.pallas_call(
            merge_kernel,
            out_shape=near((group_count, 8, seq_dev, lanes), bf16),
            in_specs=[smem, smem, vmem, vmem, vmem],
            out_specs=vmem,
            scratch_shapes=[pltpu.VMEM((seq_dev * 8, lanes), f32)],
            compiler_params=small,
        )(table_of(entry_item), table_of(entry_ok), pin(partials), pin(packed_home), pin(lse_home))
        merged = lax.all_to_all(merged, "dp", split_axis=0, concat_axis=0, tiled=True)

        sequences = group_count * seq_dev
        width_out = out_weight.shape[1]
        piece = (sequences // head_parts, width_out)
        pieces = pl.pallas_call(
            project_kernel,
            out_shape=(near(piece, bf16),) * head_parts,
            in_specs=[vmem, vmem, vmem],
            out_specs=(vmem,) * head_parts,
            scratch_shapes=[
                pltpu.VMEM((head_parts,) + piece, bf16),
            ],
            compiler_params=small,
        )(pin(merged), pin(blocks), out_weight)
        total = pieces[0].astype(f32)
        for step in reversed(range(1, head_parts)):
            ring = [(source, partner(source, step)) for source in range(head_parts)]
            total = total + lax.ppermute(pieces[step], "mp", ring).astype(f32)
        return total.astype(bf16)

    placed = (
        P("dp", "mp", None),
        P("dp", None, "mp", None),
        P("dp", None, None, None, "mp", None),
        P("mp", None, None),
        P("mp", None, None),
        P(),
        P(),
        P("mp", "dp"),
    )
    return jax.shard_map(body, mesh=mesh, in_specs=placed, out_specs=P("mp", "dp"), check_vma=False)
```

```python
import math

import jax
import jax.numpy as jnp
from jax import lax
from jax.experimental import pallas as pl
from jax.experimental.pallas import tpu as pltpu
from jax.sharding import PartitionSpec as P

very_low = -1e30
f32 = jnp.float32
bf16 = jnp.bfloat16
lanes = 128
half = 64
pad_heads = 16
stat_lanes = 16
batch = 8
batches = (24,)
sequence_unit = 1 << 10
item_unit = 1 << 22
early_bytes = 3 << 20


def three_terms(value):
    high = value.astype(bf16)
    rest = value - high.astype(f32)
    middle = rest.astype(bf16)
    low = (rest - middle.astype(f32)).astype(bf16)
    return high, middle, low


def absorbed_queries(query_rows, key_up, kv_heads):
    scale = math.log2(math.e) / math.sqrt(key_up.shape[1])
    product = lax.dot_general(
        query_rows, key_up, (((1,), (1,)), ((), ())), preferred_element_type=f32
    )
    lane = lax.broadcasted_iota(jnp.int32, (1, 1, lanes), 2)
    if kv_heads == 2:
        product = product.reshape(-1, 2, 8, lanes)
        first = product[:, 0]
        second = pltpu.roll(product[:, 1].reshape(-1, lanes), half, 1).reshape(first.shape)
    else:
        product = jnp.concatenate([product, jnp.zeros_like(product)], axis=1)
        first = product.reshape(-1, 8, lanes)
        second = jnp.zeros_like(first)
    both = jnp.concatenate([first, second], axis=1)
    both = jnp.where(lane < half, both * scale, 0.0)
    return jnp.concatenate(three_terms(both), axis=1)


def attend_all(query_terms, latents, valid):
    pairs = range(0, len(latents), 2)
    rows = query_terms[0].shape[0]
    beside = [jnp.concatenate([latents[at], latents[at + 1]], axis=1) for at in pairs]
    scores = []
    for at, latent in zip(pairs, beside):
        none = jnp.zeros_like(query_terms[at])
        terms = jnp.concatenate(
            [
                jnp.concatenate([query_terms[at], none], axis=1),
                jnp.concatenate([none, query_terms[at + 1]], axis=1),
            ],
            axis=0,
        )
        product = lax.dot_general(
            terms, latent, (((1,), (1,)), ((), ())), preferred_element_type=f32
        )
        for one, ok in ((product[:rows], valid[at]), (product[rows:], valid[at + 1])):
            scores.append(jnp.where(ok, one[0:16] + one[16:32] + one[32:48], very_low))
    peaks = [jnp.max(score, axis=1, keepdims=True) for score in scores]
    weights = [jnp.exp2(score - peak) for score, peak in zip(scores, peaks)]
    split = []
    for weight in weights:
        high = weight.astype(bf16)
        low = (weight - high.astype(f32)).astype(bf16)
        split += [high, low]
    sums = []
    for at, latent in zip(pairs, beside):
        both = jnp.dot(
            jnp.concatenate(split[2 * at : 2 * at + 4], axis=0), latent,
            preferred_element_type=f32,
        )
        sums += [both[:32, :lanes], both[32:, lanes:]]
    totals = [jnp.sum(weight, axis=1, keepdims=True) for weight in weights]
    lane = lax.broadcasted_iota(jnp.int32, (8, lanes), 1)
    packed = []
    for weighted, total in zip(sums, totals):
        weighted = (weighted[0:16] + weighted[16:32]) / total
        packed.append(
            jnp.where(lane < half, pltpu.roll(weighted[0:8], half, 1), weighted[8:16])
        )
    return packed, [peak + jnp.log2(total) for peak, total in zip(peaks, totals)]


def spread(value):
    lane = lax.broadcasted_iota(jnp.int32, (8, lanes), 1)
    return jnp.where(lane < half, value[0:8], value[8:16])


def row_masks(rows, kv_heads):
    column = lax.broadcasted_iota(jnp.int32, (pad_heads, rows), 1)
    head = lax.broadcasted_iota(jnp.int32, (pad_heads, rows), 0) // 8
    if kv_heads == 1:
        return column, head == 0
    return column // 2, (column % 2) == head


def pin(array):
    return pltpu.with_memory_space_constraint(array, pltpu.VMEM)


def table_of(array):
    return pltpu.with_memory_space_constraint(array, pltpu.SMEM)


def far(array):
    return pltpu.with_memory_space_constraint(array, pltpu.HBM)


def near(shape, kind):
    return pltpu.VMEM(shape, kind)


def solution(mesh):
    group_count = mesh.shape["dp"]
    head_parts = mesh.shape["mp"]

    def partner(source, step):
        paired = head_parts & (head_parts - 1) == 0
        return source ^ step if paired else (source + step) % head_parts

    def home_kernel(
        routes, lengths, queries, key_up, value_up, resident_far, overflow,
        page_list, page_count, entry_item, entry_ok,
        packed_out, lse_out, value_near, key_near, pages,
        holder_counts, resident, home_sem, sems,
    ):
        seq_dev, rows, _ = resident.shape
        home_copy = pltpu.make_async_copy(resident_far, resident, home_sem)
        home_copy.start()
        kv_heads = key_up.shape[0] // half
        items = overflow.shape[0]
        slots = items // group_count
        tail_pages = routes.shape[0]
        home_tokens = rows // kv_heads
        page = lanes
        me = lax.axis_index("dp")

        def scan_group(group, found):
            slot = jnp.int32(0)
            holder_counts[group] = 0
            for row in range(seq_dev):
                sequence = group * seq_dev + row
                length = lengths[sequence]
                label = group * (slots * item_unit) + sequence * sequence_unit
                for place in range(tail_pages):
                    tokens = jnp.minimum(length - (home_tokens + place * page), page)
                    named = routes[place, 0, sequence] == me
                    page_list[found] = slot * item_unit + (label + tokens)
                    slot = slot + named.astype(jnp.int32)
                    found = found + (named & (tokens > 0)).astype(jnp.int32)
            return found

        found_count = lax.fori_loop(0, group_count, scan_group, jnp.int32(0))
        page_count[0] = found_count

        def page_copy(place):
            item = page_list[place] // item_unit
            return pltpu.make_async_copy(overflow.at[item], pages.at[place], sems.at[place])

        def start_copy(place, _):
            page_copy(place).start()
            return 0

        def end_copy(place, _):
            page_copy(place).wait()
            return 0

        early_count = jnp.minimum(found_count, pages.shape[0])
        lax.fori_loop(0, early_count, start_copy, 0)
        home_copy.wait()
        for row in range(seq_dev):
            length = lengths[me * seq_dev + row]
            for place in range(tail_pages):
                entry = row * tail_pages + place
                holder = routes[place, 0, me * seq_dev + row]
                slot = holder_counts[holder]
                holder_counts[holder] = slot + 1
                entry_item[entry] = holder * slots + slot
                entry_ok[entry] = (home_tokens + place * page < length).astype(jnp.int32)
        key_near[...] = key_up[...]
        value_near[...] = value_up[...]
        terms = absorbed_queries(queries[...], key_up[...], kv_heads)
        token, head_ok = row_masks(rows, kv_heads)
        for start in range(0, seq_dev, 4):
            part = range(start, min(start + 4, seq_dev))
            packed, lse = attend_all(
                [terms[row] for row in part],
                [resident[row] for row in part],
                [head_ok & (token < lengths[me * seq_dev + row]) for row in part],
            )
            for place, row in enumerate(part):
                packed_out[row] = packed[place]
                lse_out[row] = spread(lse[place])
        lax.fori_loop(0, early_count, end_copy, 0)

    def page_kernel(
        page_list, page_count, queries, key_up, pages, overflow,
        out, terms_ref, stats_ref, *late,
    ):
        early, rows, _ = pages.shape
        items = overflow.shape[0]
        slots = items // group_count
        kv_heads = key_up.shape[0] // half
        found = page_count[0]

        def late_copy(place):
            late_pages, sems = late
            item = page_list[place] // item_unit
            at = place - early
            return pltpu.make_async_copy(overflow.at[item], late_pages.at[at], sems.at[at])

        def start_copy(place, _):
            late_copy(place).start()
            return 0

        def end_copy(place, _):
            late_copy(place).wait()
            return 0

        if late:
            lax.fori_loop(early, found, start_copy, 0)
        terms_ref[...] = absorbed_queries(queries[...], key_up[...], kv_heads)
        token, head_ok = row_masks(rows, kv_heads)
        stat_lane = lax.broadcasted_iota(jnp.int32, (pad_heads, lanes), 1)
        stat_head = lax.broadcasted_iota(jnp.int32, (pad_heads, lanes), 0) // 8
        stat_lane = stat_lane - stat_head * (stat_lanes // 2)

        def one_batch(first, size, source, shift):
            places = [jnp.minimum(first + offset, found - 1) for offset in range(size)]
            labels = [page_list[place] for place in places]
            chosen = [label // item_unit for label in labels]
            packed, lse = attend_all(
                [terms_ref[label % item_unit // sequence_unit] for label in labels],
                [source[place - shift] for place in places],
                [head_ok & (token < label % sequence_unit) for label in labels],
            )
            for offset, item in enumerate(chosen):
                group = item // slots
                slot = item - group * slots
                out[group, slot] = packed[offset].astype(bf16)
                stats = stats_ref[group]
                for place, term in enumerate(three_terms(lse[offset])):
                    mine = stat_lane == slot * stat_lanes + place
                    stats = jnp.where(mine, term.astype(f32), stats)
                stats_ref[group] = stats

        sizes = sorted({size for size in batches if size < early} | {early})
        for before, size in zip([0] + sizes, sizes):
            fits = (found > before) & (found <= size)
            if size == early:
                fits = found > before

            @pl.when(fits)
            def _(size=size):
                one_batch(0, size, pages, 0)

        def late_batch(step, _):
            one_batch(early + step * batch, batch, late[0], early)
            return 0

        if late:
            @pl.when(found > early)
            def _():
                lax.fori_loop(early, found, end_copy, 0)
                lax.fori_loop(0, (found - early + batch - 1) // batch, late_batch, 0)

        lane = lax.broadcasted_iota(jnp.int32, (group_count, 8, lanes), 2)
        stats = jnp.where(
            lane % stat_lanes < stat_lanes // 2, stats_ref[:, 0:8], stats_ref[:, 8:16]
        )
        out[:, slots] = stats.astype(bf16)

    def merge_kernel(entry_item, entry_ok, received, packed_home, lse_home, out, rows_ref):
        seq_dev = packed_home.shape[0]
        slots = received.shape[1] - 1
        tail_pages = entry_item.shape[0] // seq_dev
        lane = lax.broadcasted_iota(jnp.int32, (8, lanes), 1)
        place = lane % stat_lanes
        slot_of_lane = lane // stat_lanes
        for row in range(seq_dev):
            parts = [(lse_home[row], packed_home[row])]
            for page_index in range(tail_pages):
                entry = row * tail_pages + page_index
                item = entry_item[entry]
                holder = item // slots
                slot = item - holder * slots
                stats = jnp.where(slot_of_lane == slot, received[holder, slots].astype(f32), 0.0)
                pair = [
                    jnp.sum(
                        jnp.where((place >= start) & (place < start + 3), stats, 0.0),
                        axis=1, keepdims=True,
                    )
                    for start in (0, stat_lanes // 2)
                ]
                ok = entry_ok[entry] > 0
                lse = jnp.where(ok, jnp.where(lane < half, pair[0], pair[1]), very_low)
                packed = jnp.where(ok, received[holder, slot].astype(f32), 0.0)
                parts.append((lse, packed))
            peak = parts[0][0]
            for lse, _ in parts[1:]:
                peak = jnp.maximum(peak, lse)
            total = jnp.zeros((8, lanes), f32)
            merged = jnp.zeros((8, lanes), f32)
            for lse, packed in parts:
                factor = jnp.exp2(lse - peak)
                total = total + factor
                merged = merged + factor * packed
            rows_ref[row * 8 : (row + 1) * 8, :] = merged / total
        for query in range(8):
            block = rows_ref[pl.ds(query, seq_dev, stride=8), :].astype(bf16)
            for target in range(group_count):
                out[target, query] = block

    def project_kernel(received, value_up, weight, *rest):
        outs, out = rest[:head_parts], rest[head_parts]
        me = lax.axis_index("mp")
        sequences = received.shape[0] * received.shape[2]
        kv_heads = value_up.shape[0]
        blank = jnp.zeros((half, lanes), bf16)
        blocks = jnp.concatenate(
            [
                jnp.concatenate(
                    [value_up[head] if head == across else blank for across in range(kv_heads)],
                    axis=1,
                )
                for head in range(kv_heads)
            ]
            + [jnp.zeros((half, kv_heads * lanes), bf16)] * (2 - kv_heads),
            axis=0,
        )
        pieces = [
            jnp.dot(
                received[:, query].astype(f32).reshape(sequences, lanes).astype(bf16),
                blocks,
                preferred_element_type=f32,
            )
            for query in range(8)
        ]
        attended = jnp.concatenate(
            [
                piece[:, head * lanes : (head + 1) * lanes]
                for head in range(kv_heads)
                for piece in pieces
            ],
            axis=1,
        )
        high = attended.astype(bf16)
        low = (attended - high.astype(f32)).astype(bf16)
        both = jnp.concatenate([high, low], axis=0)
        result = jnp.dot(both, weight[...], preferred_element_type=f32)
        out[...] = (result[:sequences] + result[sequences:]).astype(bf16).reshape(out.shape)
        for step in range(head_parts):
            outs[step][...] = out[partner(me, step)]

    def body(
        queries, resident_cache, overflow_cache, key_up_weight, value_up_weight,
        lengths, routes, out_weight,
    ):
        seq_dev, head_dev, head_size = queries.shape
        kv_heads, width, _ = key_up_weight.shape
        slots = overflow_cache.shape[2]
        page = overflow_cache.shape[3]
        items = group_count * slots
        tail_pages = routes.shape[1]
        home_tokens = resident_cache.shape[1]
        smem = pl.BlockSpec(memory_space=pltpu.SMEM)
        vmem = pl.BlockSpec(memory_space=pltpu.VMEM)
        hbm = pl.BlockSpec(memory_space=pltpu.HBM)
        small = pltpu.CompilerParams(vmem_limit_bytes=16 << 20)
        ints = lambda size: pltpu.SMEM((size,), jnp.int32)
        flat_routes = routes.transpose(1, 2, 0)
        key_up = key_up_weight.reshape(kv_heads * width, head_size)
        flat_queries = queries.reshape(seq_dev * head_dev, head_size)

        spread_queries = jnp.broadcast_to(
            flat_queries[None], (group_count,) + flat_queries.shape
        )
        all_queries = lax.all_to_all(
            spread_queries, "dp", split_axis=0, concat_axis=0, tiled=True
        ).reshape(-1, head_size)

        entries = seq_dev * tail_pages
        early = early_bytes // (page * kv_heads * lanes * 2) // batch * batch
        early = min(items, early)
        (
            page_list, page_count, entry_item, entry_ok,
            packed_home, lse_home, value_near, key_near, pages,
        ) = pl.pallas_call(
            home_kernel,
            out_shape=(
                ints(items + 1), ints(1), ints(entries), ints(entries),
                near((seq_dev, 8, lanes), f32),
                near((seq_dev, 8, lanes), f32),
                near(value_up_weight.shape, bf16),
                near(key_up.shape, bf16),
                near((early, page * kv_heads, lanes), bf16),
            ),
            in_specs=[smem, smem, vmem, vmem, vmem, hbm, hbm],
            out_specs=(smem,) * 4 + (vmem,) * 5,
            scratch_shapes=[
                pltpu.SMEM((group_count,), jnp.int32),
                pltpu.VMEM((seq_dev, home_tokens * kv_heads, lanes), bf16),
                pltpu.SemaphoreType.DMA,
                pltpu.SemaphoreType.DMA((early,)),
            ],
            compiler_params=small,
            cost_estimate=pl.CostEstimate(
                flops=200_000_000, transcendentals=0, bytes_accessed=1 << 20
            ),
        )(
            far(flat_routes), far(lengths), far(flat_queries), far(key_up),
            far(value_up_weight),
            far(resident_cache.reshape(seq_dev, home_tokens * kv_heads, lanes)),
            far(overflow_cache.reshape(items, page * kv_heads, lanes)),
        )

        late = items - early
        late_scratch = [] if late <= 0 else [
            pltpu.VMEM((late, page * kv_heads, lanes), bf16),
            pltpu.SemaphoreType.DMA((late,)),
        ]
        partials = pl.pallas_call(
            page_kernel,
            out_shape=near((group_count, slots + 1, 8, lanes), bf16),
            in_specs=[smem, smem, vmem, vmem, vmem, hbm],
            out_specs=vmem,
            scratch_shapes=[
                pltpu.VMEM((group_count * seq_dev, 48, lanes), bf16),
                pltpu.VMEM((group_count, pad_heads, lanes), f32),
            ] + late_scratch,
            compiler_params=small,
        )(
            table_of(page_list), table_of(page_count), pin(all_queries), pin(key_near),
            pin(pages), far(overflow_cache.reshape(items, page * kv_heads, lanes)),
        )
        partials = lax.all_to_all(partials, "dp", split_axis=0, concat_axis=0, tiled=True)

        merged = pl.pallas_call(
            merge_kernel,
            out_shape=near((group_count, 8, seq_dev, lanes), bf16),
            in_specs=[smem, smem, vmem, vmem, vmem],
            out_specs=vmem,
            scratch_shapes=[pltpu.VMEM((seq_dev * 8, lanes), f32)],
            compiler_params=small,
        )(table_of(entry_item), table_of(entry_ok), pin(partials), pin(packed_home), pin(lse_home))
        merged = lax.all_to_all(merged, "dp", split_axis=0, concat_axis=0, tiled=True)

        sequences = group_count * seq_dev
        width_out = out_weight.shape[1]
        piece = (sequences // head_parts, width_out)
        pieces = pl.pallas_call(
            project_kernel,
            out_shape=(near(piece, bf16),) * head_parts,
            in_specs=[vmem, vmem, vmem],
            out_specs=(vmem,) * head_parts,
            scratch_shapes=[
                pltpu.VMEM((head_parts,) + piece, bf16),
            ],
            compiler_params=small,
        )(pin(merged), pin(value_near), out_weight)
        total = pieces[0].astype(f32)
        for step in reversed(range(1, head_parts)):
            ring = [(source, partner(source, step)) for source in range(head_parts)]
            total = total + lax.ppermute(pieces[step], "mp", ring).astype(f32)
        return total.astype(bf16)

    placed = (
        P("dp", "mp", None),
        P("dp", None, "mp", None),
        P("dp", None, None, None, "mp", None),
        P("mp", None, None),
        P("mp", None, None),
        P(),
        P(),
        P("mp", "dp"),
    )
    return jax.shard_map(body, mesh=mesh, in_specs=placed, out_specs=P("mp", "dp"), check_vma=False)
```

```python
import math

import jax
import jax.numpy as jnp
from jax import lax
from jax.experimental import pallas as pl
from jax.experimental.pallas import tpu as pltpu
from jax.sharding import PartitionSpec as P

very_low = -1e30
f32 = jnp.float32
bf16 = jnp.bfloat16
lanes = 128
half = 64
pad_heads = 16
stat_lanes = 16
batch = 8
batches = (16, 24, 32, 40)
sequence_unit = 1 << 10
item_unit = 1 << 22
early_bytes = 3 << 20


def three_terms(value):
    high = value.astype(bf16)
    rest = value - high.astype(f32)
    middle = rest.astype(bf16)
    low = (rest - middle.astype(f32)).astype(bf16)
    return high, middle, low


def absorbed_queries(query_rows, key_up, kv_heads):
    scale = math.log2(math.e) / math.sqrt(key_up.shape[1])
    product = lax.dot_general(
        query_rows, key_up, (((1,), (1,)), ((), ())), preferred_element_type=f32
    )
    lane = lax.broadcasted_iota(jnp.int32, (1, 1, lanes), 2)
    if kv_heads == 2:
        product = product.reshape(-1, 2, 8, lanes)
        first = product[:, 0]
        second = pltpu.roll(product[:, 1].reshape(-1, lanes), half, 1).reshape(first.shape)
    else:
        product = jnp.concatenate([product, jnp.zeros_like(product)], axis=1)
        first = product.reshape(-1, 8, lanes)
        second = jnp.zeros_like(first)
    both = jnp.concatenate([first, second], axis=1)
    both = jnp.where(lane < half, both * scale, 0.0)
    return jnp.concatenate(three_terms(both), axis=1)


def attend_all(query_terms, latents, valid):
    pairs = range(0, len(latents), 2)
    rows = query_terms[0].shape[0]
    beside = [jnp.concatenate([latents[at], latents[at + 1]], axis=1) for at in pairs]
    scores = []
    for at, latent in zip(pairs, beside):
        none = jnp.zeros_like(query_terms[at])
        terms = jnp.concatenate(
            [
                jnp.concatenate([query_terms[at], none], axis=1),
                jnp.concatenate([none, query_terms[at + 1]], axis=1),
            ],
            axis=0,
        )
        product = lax.dot_general(
            terms, latent, (((1,), (1,)), ((), ())), preferred_element_type=f32
        )
        for one, ok in ((product[:rows], valid[at]), (product[rows:], valid[at + 1])):
            scores.append(jnp.where(ok, one[0:16] + one[16:32] + one[32:48], very_low))
    peaks = [jnp.max(score, axis=1, keepdims=True) for score in scores]
    weights = [jnp.exp2(score - peak) for score, peak in zip(scores, peaks)]
    split = []
    for weight in weights:
        high = weight.astype(bf16)
        low = (weight - high.astype(f32)).astype(bf16)
        split += [high, low]
    sums = []
    for at, latent in zip(pairs, beside):
        both = jnp.dot(
            jnp.concatenate(split[2 * at : 2 * at + 4], axis=0), latent,
            preferred_element_type=f32,
        )
        sums += [both[:32, :lanes], both[32:, lanes:]]
    totals = [jnp.sum(weight, axis=1, keepdims=True) for weight in weights]
    lane = lax.broadcasted_iota(jnp.int32, (8, lanes), 1)
    packed = []
    for weighted, total in zip(sums, totals):
        weighted = (weighted[0:16] + weighted[16:32]) / total
        packed.append(
            jnp.where(lane < half, pltpu.roll(weighted[0:8], half, 1), weighted[8:16])
        )
    return packed, [peak + jnp.log2(total) for peak, total in zip(peaks, totals)]


def spread(value):
    lane = lax.broadcasted_iota(jnp.int32, (8, lanes), 1)
    return jnp.where(lane < half, value[0:8], value[8:16])


def row_masks(rows, kv_heads):
    column = lax.broadcasted_iota(jnp.int32, (pad_heads, rows), 1)
    head = lax.broadcasted_iota(jnp.int32, (pad_heads, rows), 0) // 8
    if kv_heads == 1:
        return column, head == 0
    return column // 2, (column % 2) == head


def pin(array):
    return pltpu.with_memory_space_constraint(array, pltpu.VMEM)


def table_of(array):
    return pltpu.with_memory_space_constraint(array, pltpu.SMEM)


def far(array):
    return pltpu.with_memory_space_constraint(array, pltpu.HBM)


def near(shape, kind):
    return pltpu.VMEM(shape, kind)


def solution(mesh):
    group_count = mesh.shape["dp"]
    head_parts = mesh.shape["mp"]

    def partner(source, step):
        paired = head_parts & (head_parts - 1) == 0
        return source ^ step if paired else (source + step) % head_parts

    def home_kernel(
        routes, lengths, queries, key_up, value_up, resident_far, overflow,
        page_list, page_count, entry_item, entry_ok,
        packed_out, lse_out, value_near, key_near, pages,
        holder_counts, resident, home_sem, sems,
    ):
        seq_dev, rows, _ = resident.shape
        home_copy = pltpu.make_async_copy(resident_far, resident, home_sem)
        home_copy.start()
        kv_heads = key_up.shape[0] // half
        items = overflow.shape[0]
        slots = items // group_count
        tail_pages = routes.shape[0]
        home_tokens = rows // kv_heads
        page = lanes
        me = lax.axis_index("dp")

        def page_copy(place):
            item = page_list[place] // item_unit
            return pltpu.make_async_copy(overflow.at[item], pages.at[place], sems.at[place])

        def start_copy(place, _):
            page_copy(place).start()
            return 0

        def end_copy(place, _):
            page_copy(place).wait()
            return 0

        early = pages.shape[0]

        def scan_group(group, found):
            before = jnp.minimum(found, early)
            slot = jnp.int32(0)
            holder_counts[group] = 0
            for row in range(seq_dev):
                sequence = group * seq_dev + row
                length = lengths[sequence]
                label = group * (slots * item_unit) + sequence * sequence_unit
                for place in range(tail_pages):
                    tokens = jnp.minimum(length - (home_tokens + place * page), page)
                    named = routes[place, 0, sequence] == me
                    page_list[found] = slot * item_unit + (label + tokens)
                    slot = slot + named.astype(jnp.int32)
                    found = found + (named & (tokens > 0)).astype(jnp.int32)
            lax.fori_loop(before, jnp.minimum(found, early), start_copy, 0)
            return found

        found_count = lax.fori_loop(0, group_count, scan_group, jnp.int32(0))
        page_count[0] = found_count

        early_count = jnp.minimum(found_count, early)
        home_copy.wait()
        for row in range(seq_dev):
            length = lengths[me * seq_dev + row]
            for place in range(tail_pages):
                entry = row * tail_pages + place
                holder = routes[place, 0, me * seq_dev + row]
                slot = holder_counts[holder]
                holder_counts[holder] = slot + 1
                entry_item[entry] = holder * slots + slot
                entry_ok[entry] = (home_tokens + place * page < length).astype(jnp.int32)
        key_near[...] = key_up[...]
        value_near[...] = value_up[...]
        terms = absorbed_queries(queries[...], key_up[...], kv_heads)
        token, head_ok = row_masks(rows, kv_heads)
        for start in range(0, seq_dev, 4):
            part = range(start, min(start + 4, seq_dev))
            packed, lse = attend_all(
                [terms[row] for row in part],
                [resident[row] for row in part],
                [head_ok & (token < lengths[me * seq_dev + row]) for row in part],
            )
            for place, row in enumerate(part):
                packed_out[row] = packed[place]
                lse_out[row] = spread(lse[place])
        lax.fori_loop(0, early_count, end_copy, 0)

    def page_kernel(
        page_list, page_count, queries, key_up, pages, overflow,
        out, terms_ref, stats_ref, *late,
    ):
        early, rows, _ = pages.shape
        items = overflow.shape[0]
        slots = items // group_count
        kv_heads = key_up.shape[0] // half
        found = page_count[0]

        def late_copy(place):
            late_pages, sems = late
            item = page_list[place] // item_unit
            at = place - early
            return pltpu.make_async_copy(overflow.at[item], late_pages.at[at], sems.at[at])

        def start_copy(place, _):
            late_copy(place).start()
            return 0

        def end_copy(place, _):
            late_copy(place).wait()
            return 0

        if late:
            lax.fori_loop(early, found, start_copy, 0)
        terms_ref[...] = absorbed_queries(queries[...], key_up[...], kv_heads)
        token, head_ok = row_masks(rows, kv_heads)
        stat_lane = lax.broadcasted_iota(jnp.int32, (pad_heads, lanes), 1)
        stat_head = lax.broadcasted_iota(jnp.int32, (pad_heads, lanes), 0) // 8
        stat_lane = stat_lane - stat_head * (stat_lanes // 2)

        def one_batch(first, size, source, shift):
            places = [jnp.minimum(first + offset, found - 1) for offset in range(size)]
            labels = [page_list[place] for place in places]
            chosen = [label // item_unit for label in labels]
            packed, lse = attend_all(
                [terms_ref[label % item_unit // sequence_unit] for label in labels],
                [source[place - shift] for place in places],
                [head_ok & (token < label % sequence_unit) for label in labels],
            )
            for offset, item in enumerate(chosen):
                group = item // slots
                slot = item - group * slots
                out[group, slot] = packed[offset].astype(bf16)
                stats = stats_ref[group]
                for place, term in enumerate(three_terms(lse[offset])):
                    mine = stat_lane == slot * stat_lanes + place
                    stats = jnp.where(mine, term.astype(f32), stats)
                stats_ref[group] = stats

        sizes = sorted({size for size in batches if size < early} | {early})
        for before, size in zip([0] + sizes, sizes):
            fits = (found > before) & (found <= size)
            if size == early:
                fits = found > before

            @pl.when(fits)
            def _(size=size):
                one_batch(0, size, pages, 0)

        def late_batch(step, _):
            one_batch(early + step * batch, batch, late[0], early)
            return 0

        if late:
            @pl.when(found > early)
            def _():
                lax.fori_loop(early, found, end_copy, 0)
                lax.fori_loop(0, (found - early + batch - 1) // batch, late_batch, 0)

        lane = lax.broadcasted_iota(jnp.int32, (group_count, 8, lanes), 2)
        stats = jnp.where(
            lane % stat_lanes < stat_lanes // 2, stats_ref[:, 0:8], stats_ref[:, 8:16]
        )
        out[:, slots] = stats.astype(bf16)

    def merge_kernel(entry_item, entry_ok, received, packed_home, lse_home, out, rows_ref):
        seq_dev = packed_home.shape[0]
        slots = received.shape[1] - 1
        tail_pages = entry_item.shape[0] // seq_dev
        lane = lax.broadcasted_iota(jnp.int32, (8, lanes), 1)
        place = lane % stat_lanes
        slot_of_lane = lane // stat_lanes
        for row in range(seq_dev):
            parts = [(lse_home[row], packed_home[row])]
            for page_index in range(tail_pages):
                entry = row * tail_pages + page_index
                item = entry_item[entry]
                holder = item // slots
                slot = item - holder * slots
                stats = jnp.where(slot_of_lane == slot, received[holder, slots].astype(f32), 0.0)
                pair = [
                    jnp.sum(
                        jnp.where((place >= start) & (place < start + 3), stats, 0.0),
                        axis=1, keepdims=True,
                    )
                    for start in (0, stat_lanes // 2)
                ]
                ok = entry_ok[entry] > 0
                lse = jnp.where(ok, jnp.where(lane < half, pair[0], pair[1]), very_low)
                packed = jnp.where(ok, received[holder, slot].astype(f32), 0.0)
                parts.append((lse, packed))
            peak = parts[0][0]
            for lse, _ in parts[1:]:
                peak = jnp.maximum(peak, lse)
            total = jnp.zeros((8, lanes), f32)
            merged = jnp.zeros((8, lanes), f32)
            for lse, packed in parts:
                factor = jnp.exp2(lse - peak)
                total = total + factor
                merged = merged + factor * packed
            rows_ref[row * 8 : (row + 1) * 8, :] = merged / total
        for query in range(8):
            block = rows_ref[pl.ds(query, seq_dev, stride=8), :].astype(bf16)
            for target in range(group_count):
                out[target, query] = block

    def project_kernel(received, value_up, weight, *rest):
        outs, out = rest[:head_parts], rest[head_parts]
        me = lax.axis_index("mp")
        sequences = received.shape[0] * received.shape[2]
        kv_heads = value_up.shape[0]
        blank = jnp.zeros((half, lanes), bf16)
        blocks = jnp.concatenate(
            [
                jnp.concatenate(
                    [value_up[head] if head == across else blank for across in range(kv_heads)],
                    axis=1,
                )
                for head in range(kv_heads)
            ]
            + [jnp.zeros((half, kv_heads * lanes), bf16)] * (2 - kv_heads),
            axis=0,
        )
        pieces = [
            jnp.dot(
                received[:, query].astype(f32).reshape(sequences, lanes).astype(bf16),
                blocks,
                preferred_element_type=f32,
            )
            for query in range(8)
        ]
        attended = jnp.concatenate(
            [
                piece[:, head * lanes : (head + 1) * lanes]
                for head in range(kv_heads)
                for piece in pieces
            ],
            axis=1,
        )
        high = attended.astype(bf16)
        low = (attended - high.astype(f32)).astype(bf16)
        both = jnp.concatenate([high, low], axis=0)
        result = jnp.dot(both, weight[...], preferred_element_type=f32)
        out[...] = (result[:sequences] + result[sequences:]).astype(bf16).reshape(out.shape)
        for step in range(head_parts):
            outs[step][...] = out[partner(me, step)]

    def body(
        queries, resident_cache, overflow_cache, key_up_weight, value_up_weight,
        lengths, routes, out_weight,
    ):
        seq_dev, head_dev, head_size = queries.shape
        kv_heads, width, _ = key_up_weight.shape
        slots = overflow_cache.shape[2]
        page = overflow_cache.shape[3]
        items = group_count * slots
        tail_pages = routes.shape[1]
        home_tokens = resident_cache.shape[1]
        smem = pl.BlockSpec(memory_space=pltpu.SMEM)
        vmem = pl.BlockSpec(memory_space=pltpu.VMEM)
        hbm = pl.BlockSpec(memory_space=pltpu.HBM)
        small = pltpu.CompilerParams(vmem_limit_bytes=16 << 20)
        ints = lambda size: pltpu.SMEM((size,), jnp.int32)
        flat_routes = routes.transpose(1, 2, 0)
        key_up = key_up_weight.reshape(kv_heads * width, head_size)
        flat_queries = queries.reshape(seq_dev * head_dev, head_size)

        spread_queries = jnp.broadcast_to(
            flat_queries[None], (group_count,) + flat_queries.shape
        )
        all_queries = lax.all_to_all(
            spread_queries, "dp", split_axis=0, concat_axis=0, tiled=True
        ).reshape(-1, head_size)

        entries = seq_dev * tail_pages
        early = early_bytes // (page * kv_heads * lanes * 2) // batch * batch
        early = min(items, early)
        (
            page_list, page_count, entry_item, entry_ok,
            packed_home, lse_home, value_near, key_near, pages,
        ) = pl.pallas_call(
            home_kernel,
            out_shape=(
                ints(items + 1), ints(1), ints(entries), ints(entries),
                near((seq_dev, 8, lanes), f32),
                near((seq_dev, 8, lanes), f32),
                near(value_up_weight.shape, bf16),
                near(key_up.shape, bf16),
                near((early, page * kv_heads, lanes), bf16),
            ),
            in_specs=[smem, smem, vmem, vmem, vmem, hbm, hbm],
            out_specs=(smem,) * 4 + (vmem,) * 5,
            scratch_shapes=[
                pltpu.SMEM((group_count,), jnp.int32),
                pltpu.VMEM((seq_dev, home_tokens * kv_heads, lanes), bf16),
                pltpu.SemaphoreType.DMA,
                pltpu.SemaphoreType.DMA((early,)),
            ],
            compiler_params=small,
            cost_estimate=pl.CostEstimate(
                flops=200_000_000, transcendentals=0, bytes_accessed=1 << 20
            ),
        )(
            far(flat_routes), far(lengths), far(flat_queries), far(key_up),
            far(value_up_weight),
            far(resident_cache.reshape(seq_dev, home_tokens * kv_heads, lanes)),
            far(overflow_cache.reshape(items, page * kv_heads, lanes)),
        )

        late = items - early
        late_scratch = [] if late <= 0 else [
            pltpu.VMEM((late, page * kv_heads, lanes), bf16),
            pltpu.SemaphoreType.DMA((late,)),
        ]
        partials = pl.pallas_call(
            page_kernel,
            out_shape=near((group_count, slots + 1, 8, lanes), bf16),
            in_specs=[smem, smem, vmem, vmem, vmem, hbm],
            out_specs=vmem,
            scratch_shapes=[
                pltpu.VMEM((group_count * seq_dev, 48, lanes), bf16),
                pltpu.VMEM((group_count, pad_heads, lanes), f32),
            ] + late_scratch,
            compiler_params=small,
        )(
            table_of(page_list), table_of(page_count), pin(all_queries), pin(key_near),
            pin(pages), far(overflow_cache.reshape(items, page * kv_heads, lanes)),
        )
        partials = lax.all_to_all(partials, "dp", split_axis=0, concat_axis=0, tiled=True)

        merged = pl.pallas_call(
            merge_kernel,
            out_shape=near((group_count, 8, seq_dev, lanes), bf16),
            in_specs=[smem, smem, vmem, vmem, vmem],
            out_specs=vmem,
            scratch_shapes=[pltpu.VMEM((seq_dev * 8, lanes), f32)],
            compiler_params=small,
        )(table_of(entry_item), table_of(entry_ok), pin(partials), pin(packed_home), pin(lse_home))
        merged = lax.all_to_all(merged, "dp", split_axis=0, concat_axis=0, tiled=True)

        sequences = group_count * seq_dev
        width_out = out_weight.shape[1]
        piece = (sequences // head_parts, width_out)
        pieces = pl.pallas_call(
            project_kernel,
            out_shape=(near(piece, bf16),) * head_parts,
            in_specs=[vmem, vmem, vmem],
            out_specs=(vmem,) * head_parts,
            scratch_shapes=[
                pltpu.VMEM((head_parts,) + piece, bf16),
            ],
            compiler_params=small,
        )(pin(merged), pin(value_near), out_weight)
        total = pieces[0].astype(f32)
        for step in reversed(range(1, head_parts)):
            ring = [(source, partner(source, step)) for source in range(head_parts)]
            total = total + lax.ppermute(pieces[step], "mp", ring).astype(f32)
        return total.astype(bf16)

    placed = (
        P("dp", "mp", None),
        P("dp", None, "mp", None),
        P("dp", None, None, None, "mp", None),
        P("mp", None, None),
        P("mp", None, None),
        P(),
        P(),
        P("mp", "dp"),
    )
    return jax.shard_map(body, mesh=mesh, in_specs=placed, out_specs=P("mp", "dp"), check_vma=False)
```
